32 devices in a mesh: node: 16 (over z, x, core), tone: 2 (over y).
Axes of the slice: x: 2, y: 2, z: 4, core: 2. Of those that a mesh axis runs over, the one named last changes fastest.
Arguments:
- voltages: float32 [32, 32, 16384], P(None, 'tone', 'node'), may hold values from -6 to 6
- source: float32 [32, 32, 16384], P(None, 'tone', 'node'), may hold values from -6 to 6
- coupling: float32 [128, 7, 128, 128], P('node'), may hold values from -0.1875 to 0.1875
- band_code: int32 [7], replicated, may hold values from 0 to 6, each once
- active: int32 [128, 7], P('node'), may hold values 0 or 1
- cap: float32 [16384], P('node'), may hold values from 0.5 to 2
- damp: float32 [32, 32], P(None, 'tone'), may hold values from 0.5 to 4
- kind: int32 [16384], P('node'), may hold values from 0 to 3
- type_params: float32 [3, 4], replicated, may hold values from 0.3 to 2
Outputs:
- new_voltages: float32 [32, 32, 16384], P(None, 'tone', 'node')
- remaining: float32 [32, 32, 16384], P(None, 'tone', 'node')
The draws below stay inside these ranges and needn't reach their ends.
Inputs may be any that keep to these rules, and one draw needn't show every extreme that they name: band_code holds each of 0 to 6 once, so the bands reach every block offset from -3 to 3.
All inputs are finite; a program needn't handle non-finite values. No bound on the sum of `active` on one device may be relied on, other than what follows from the above.
Results may differ from the reference program's by a relative error of at most 0.0003.
Values sent between devices are 32-bit elements; how exact they have to be, the bound alone decides.
No kernel may reach another device: no remote copies, remote signals or barrier semaphores. Data moves between devices by JAX's collectives and lax.ppermute only.
A program may use at most 128 MiB of HBM per device.

```python
import math
import jax
import jax.numpy as jnp
from jax import lax

K1 = 32
K2 = 32
NB = 128
HALO_B = 3
NOFF = 7
M = 4
NTYPES = 4
NODES = 16384
NBLOCKS = 128


def set_ends(entries, key, low, largest):
    place = [jax.random.randint(jax.random.fold_in(key, axis), (), 0, length) for axis, length in enumerate(entries.shape)]
    longest = entries.shape.index(max(entries.shape))
    beside = place[:longest] + [(place[longest] + 1) % entries.shape[longest]] + place[longest + 1:]
    return entries.at[tuple(place)].set(low).at[tuple(beside)].set(largest)


def level_of(rng, dims, pieces, low, high):
    loudness = 1.0
    for position, blocks in pieces:
        steps = jax.random.uniform(jax.random.fold_in(jax.random.fold_in(rng, 6), position), (blocks,), jnp.float32, low / len(pieces), high / len(pieces))
        loudness = loudness * jnp.repeat(jnp.exp(steps), dims[position] // blocks).reshape((-1,) + (1,) * (len(dims) - 1 - position))
    return loudness


def scatter_about(own_key, dims, width, limit, shards=(), kind=jnp.bfloat16):
    array = width * jax.random.normal(own_key, dims, jnp.float32)
    if shards:
        array = array * level_of(own_key, dims, shards, -0.22, 0.18)
    return jnp.clip(array, -limit, limit).astype(kind)


def setup_inputs(seed: int = 0) -> dict:
    keys = jax.random.split(jax.random.key(seed), 10)
    voltages = scatter_about(keys[0], (K1, K2, NODES), 1.0, 6.0, ((1, 2), (2, 16)), jnp.float32)
    source = scatter_about(keys[1], (K1, K2, NODES), 1.0, 6.0, ((1, 2), (2, 16)), jnp.float32)
    coupling = scatter_about(keys[2], (NBLOCKS, NOFF, NB, NB), (NB * NOFF) ** -0.5, 0.1875, ((0, 16),), jnp.float32)
    band_code = jax.random.permutation(keys[3], NOFF).astype(jnp.int32)
    active = set_ends((jax.random.randint(keys[4], (NBLOCKS, NOFF), 0, 4) < 3).astype(jnp.int32), jax.random.fold_in(keys[4], 1), 0, 1)
    cap = jnp.clip(jnp.exp(math.log(2.0) - 1.3862944 * jax.random.uniform(keys[5], (NODES,), jnp.float32) ** level_of(keys[5], (NODES,), ((0, 16),), -0.2, 0.2)), 0.5, 2.0)
    damp = jnp.clip(jnp.exp(math.log(4.0) - 2.0794415 * jax.random.uniform(keys[6], (K1, K2), jnp.float32) ** level_of(keys[6], (K1, K2), ((1, 2),), -0.2, 0.2)), 0.5, 4.0)
    kind = set_ends(jax.random.randint(keys[7], (NODES,), 0, NTYPES), jax.random.fold_in(keys[7], 1), 0, NTYPES - 1).astype(jnp.int32)
    type_params = jnp.clip(jnp.exp(jax.random.uniform(keys[8], (3, NTYPES), jnp.float32, math.log(0.3), math.log(2.0))), 0.3, 2.0)
    return dict(voltages=voltages, source=source, coupling=coupling, band_code=band_code, active=active, cap=cap, damp=damp, kind=kind, type_params=type_params)


HIGH = lax.Precision.HIGHEST

def hartley(count):
    grid = jnp.arange(count, dtype=jnp.int32)
    phase = grid[:, None] * grid[None, :] % count
    angle = phase.astype(jnp.float32) * (2.0 * math.pi / count)
    return (jnp.cos(angle) + jnp.sin(angle)) / math.sqrt(count)

def transform(field, first, second):
    field = jnp.einsum('tk,kqn->tqn', first, field, precision=HIGH)
    return jnp.einsum('sq,tqn->tsn', second, field, precision=HIGH)

def couple(field, masked, band_code, scale):
    nodes = field.shape[2]
    blocks = nodes // NB
    reach = HALO_B * NB
    padded = jnp.pad(field, ((0, 0), (0, 0), (reach, reach)))
    rows = field.shape[0] * field.shape[1]
    total = scale * field
    for band in range(NOFF):
        begin = (band_code[band] * NB).astype(jnp.int32)
        source = lax.dynamic_slice_in_dim(padded, begin, nodes, 2)
        term = jnp.einsum('rbc,bsc->rbs', source.reshape(rows, blocks, NB), masked[:, band], precision=HIGH)
        total = total + term.reshape(field.shape)
    return total

def small_solve(gram, rhs):
    lower = jnp.linalg.cholesky(gram)
    count = rhs.shape[0]
    forward = []
    for index in range(count):
        total = rhs[index]
        for other in range(index):
            total = total - lower[index, other] * forward[other]
        forward.append(total / lower[index, index])
    backward = [None] * count
    for index in reversed(range(count)):
        total = forward[index]
        for other in range(index + 1, count):
            total = total - lower[other, index] * backward[other]
        backward[index] = total / lower[index, index]
    return jnp.stack(backward)

def reference(voltages, source, coupling, band_code, active, cap, damp, kind, type_params):
    first = hartley(K1)
    second = hartley(K2)
    onehot = (kind[None, :] == jnp.arange(NTYPES, dtype=jnp.int32)[:, None]).astype(type_params.dtype)
    per_node = jnp.dot(type_params, onehot, precision=HIGH)
    linear, amplitude, sharpness = (per_node[0], per_node[1], per_node[2])
    masked = coupling * active[:, :, None, None].astype(coupling.dtype)
    scale = damp[:, :, None] * cap[None, None, :]
    wave = transform(voltages, first, second)
    bend = jnp.tanh(sharpness * wave)
    current = linear * wave + amplitude * bend
    slope = linear + amplitude * sharpness * (1.0 - bend * bend)
    start = source - couple(voltages, masked, band_code, scale) - transform(current, first, second)

    def jacobian(field):
        return couple(field, masked, band_code, scale) + transform(slope * transform(field, first, second), first, second)
    beta = jnp.sqrt(jnp.sum(start * start))
    basis = [start / beta]
    hessen = jnp.zeros((M + 1, M), dtype=start.dtype)
    for column in range(M):
        image = jacobian(basis[column])
        projected = jnp.stack([jnp.sum(vector * image) for vector in basis])
        for index in range(len(basis)):
            image = image - projected[index] * basis[index]
        length = jnp.sqrt(jnp.sum(image * image))
        hessen = hessen.at[:column + 1, column].set(projected)
        hessen = hessen.at[column + 1, column].set(length)
        basis.append(image / length)
    gram = jnp.dot(hessen.T, hessen, precision=HIGH)
    coeffs = small_solve(gram, beta * hessen[0])
    fitted = jnp.dot(hessen, coeffs, precision=HIGH)
    update = coeffs[0] * basis[0]
    for index in range(1, M):
        update = update + coeffs[index] * basis[index]
    remaining = start
    for index in range(M + 1):
        remaining = remaining - fitted[index] * basis[index]
    return (voltages + update, remaining)
```

```python
import functools
import math

import jax
import jax.numpy as jnp
from jax import lax
from jax.experimental import pallas as pl
from jax.experimental.pallas import tpu as pltpu
from jax.sharding import PartitionSpec as P

NB = 128
HALO_B = 3
NOFF = 7
M = 4
NTYPES = 4
AXES = ("node", "tone")
EXACT = lax.Precision.HIGHEST
F32 = jnp.float32
BF16 = jnp.bfloat16
LIMIT = 16 * 1024 * 1024
ROWS = 128


class Chain:
    def __init__(self, nodes, tones):
        self.nodes, self.tones = nodes, tones
        self.at = [0] * (nodes * tones)
        for i in range(nodes):
            for t in range(tones):
                place = (i // 2) * 2 * tones + 2 * self.turn(i, t) + i % 2
                self.at[place] = i * tones + t

    def turn(self, i, t):
        return t if (i // 2) % 2 == 0 else self.tones - 1 - t

    def device(self, group, core, turn):
        return self.at[group * 2 * self.tones + 2 * turn + core]

    def up(self, hop):
        return [(self.at[p], self.at[p + hop]) for p in range(len(self.at) - hop)]

    def down(self, hop):
        return [(b, a) for a, b in self.up(hop)]

    def node_up(self, hop):
        tones = self.tones
        return [
            (i * tones + t, (i + hop) * tones + t)
            for i in range(self.nodes - hop)
            for t in range(tones)
        ]

    def node_down(self, hop):
        return [(b, a) for a, b in self.node_up(hop)]

    def swap(self):
        tones = self.tones
        return [(i * tones + t, (i ^ 1) * tones + t) for i in range(self.nodes) for t in range(tones)]

    def shift(self, s):
        tones = self.tones
        return [
            (i * tones + t, i * tones + (t + s) % tones)
            for i in range(self.nodes)
            for t in range(tones)
        ]

    def first(self):
        pairs = []
        for g in range(self.nodes // 2):
            for a, b in (((0, 0), (1, 0)), ((0, 1), (0, 0)), ((1, 0), (1, 1)), ((1, 1), (0, 1))):
                pairs.append((self.device(g, *a), self.device(g, *b)))
        return pairs

    def second(self):
        pairs = []
        for g in range(self.nodes // 2):
            for a, b in (((0, 1), (1, 0)), ((1, 0), (0, 1))):
                pairs.append((self.device(g, *a), self.device(g, *b)))
        return pairs


def flipped(pairs):
    return [(b, a) for a, b in pairs]


def turned(tones, place, index):
    return jnp.where((place["group"] % 2) == 0, index, tones - 1 - index)


def parity_chunks(value, tones, parity, axis):
    width = value.shape[axis] // tones
    parts = [
        lax.dynamic_slice_in_dim(value, (2 * h + parity) * width, width, axis)
        for h in range(tones // 2)
    ]
    return parts[0] if len(parts) == 1 else jnp.concatenate(parts, axis=axis)


def core_swap(chain, value, core, axis):
    keep = parity_chunks(value, chain.tones, core, axis)
    give = parity_chunks(value, chain.tones, 1 - core, axis)
    got = lax.ppermute(give, AXES, chain.swap())
    return jnp.where(core == 0, keep, got), jnp.where(core == 0, got, keep)


def chunk_of(chain, value, place, axis):
    low, high = core_swap(chain, value, place["core"], axis)
    half = chain.tones // 2
    both = jnp.where(place["turn"] < half, low, high)
    width = value.shape[axis] // chain.tones
    return lax.dynamic_slice_in_dim(both, place["turn"] % half * width, width, axis)


def gather_tones(chain, field, place):
    tones, tone, core, turn = chain.tones, place["tone"], place["core"], place["turn"]
    width = field.shape[2] // tones
    rows = field.shape[0] * field.shape[1]
    field = field.reshape(rows, field.shape[2])
    if tones == 2:
        one = lax.dynamic_slice_in_dim(field, (1 - turn) * width, width, 1)
        two = lax.dynamic_slice_in_dim(field, turn * width, width, 1)
        got_one = lax.ppermute(one, AXES, chain.first())
        got_two = lax.ppermute(two, AXES, chain.second())
        same = jnp.where(core == turn, two, got_one)
        other = jnp.where(core == turn, got_one, got_two)
        return jnp.concatenate(
            [jnp.where(tone == 0, same, other), jnp.where(tone == 0, other, same)], axis=0
        )
    low, high = core_swap(chain, field, core, 1)
    chunks = jnp.concatenate([low, high], axis=1)
    out = jnp.zeros((tones * rows, width), field.dtype)
    for s in range(tones):
        target = turned(tones, place, (tone + s) % tones)
        piece = lax.dynamic_slice_in_dim(chunks, target * width, width, 1)
        if s:
            piece = lax.ppermute(piece, AXES, chain.shift(s))
        out = lax.dynamic_update_slice_in_dim(out, piece, (tone - s) % tones * rows, 0)
    return out


def scatter_tones(chain, field, place, shape):
    tones, tone, core, turn = chain.tones, place["tone"], place["core"], place["turn"]
    width = field.shape[1]
    rows = field.shape[0] // tones
    if tones == 2:
        same = lax.dynamic_slice_in_dim(field, tone * rows, rows, 0)
        other = lax.dynamic_slice_in_dim(field, (1 - tone) * rows, rows, 0)
        one = jnp.where(core == turn, other, same)
        got_one = lax.ppermute(one, AXES, flipped(chain.first()))
        got_two = lax.ppermute(other, AXES, flipped(chain.second()))
        at_turn = jnp.where(core == turn, same, got_two)
        return jnp.concatenate(
            [jnp.where(turn == 0, at_turn, got_one), jnp.where(turn == 0, got_one, at_turn)], axis=1
        ).reshape(shape)
    chunks = jnp.zeros((rows, tones * width), field.dtype)
    for s in range(tones):
        piece = lax.dynamic_slice_in_dim(field, (tone + s) % tones * rows, rows, 0)
        if s:
            piece = lax.ppermute(piece, AXES, chain.shift(s))
        slot = turned(tones, place, (tone - s) % tones)
        chunks = lax.dynamic_update_slice_in_dim(chunks, piece, slot * width, 1)
    half = tones // 2 * width
    low, high = chunks[:, :half], chunks[:, half:]
    keep = jnp.where(core == 0, low, high)
    give = jnp.where(core == 0, high, low)
    got = lax.ppermute(give, AXES, chain.swap())
    even, odd = jnp.where(core == 0, keep, got), jnp.where(core == 0, got, keep)
    parts = []
    for h in range(tones // 2):
        parts += [even[:, h * width : (h + 1) * width], odd[:, h * width : (h + 1) * width]]
    return jnp.concatenate(parts, axis=1).reshape(shape)


def edges_of(field):
    take = min(field.shape[1], HALO_B * NB)
    return field[:, field.shape[1] - take :], field[:, :take]


def halos(last, first, up, down):
    width = last.shape[1]
    reach = HALO_B * NB
    left, right = [], []
    hop, have = 1, 0
    while have < reach:
        take = min(width, reach - have)
        left.insert(0, lax.ppermute(last[:, width - take :], AXES, up(hop)))
        right.append(lax.ppermute(first[:, :take], AXES, down(hop)))
        have, hop = have + take, hop + 1
    if len(left) == 1:
        return left[0], right[0]
    return jnp.concatenate(left, axis=1), jnp.concatenate(right, axis=1)


def hartley(count):
    grid = jnp.arange(count, dtype=jnp.int32)
    phase = grid[:, None] * grid[None, :] % count
    angle = phase.astype(F32) * (2.0 * math.pi / count)
    return (jnp.cos(angle) + jnp.sin(angle)) / math.sqrt(count)


def halves(value):
    top = value.astype(BF16)
    return top, (value - top.astype(F32)).astype(BF16)


def rounded_halves(value):
    top = lax.reduce_precision(value, exponent_bits=8, mantissa_bits=7)
    return top.astype(BF16), (value - top).astype(BF16)


def two_tone_tables(k1, k2, tones):
    local, half = k2 // tones, k1 // 2
    rows = jnp.arange(half * k2 // 2, dtype=jnp.int32)
    index1 = rows // local % half
    index2 = rows // (local * half) * local + rows % local

    def spread(index, table):
        pick = (index[:, None] == jnp.arange(table.shape[0], dtype=jnp.int32)[None, :]).astype(F32)
        left = jnp.dot(pick, table, precision=EXACT)
        return lax.dot_general(left, pick, (((1,), (1,)), ((), ())), precision=EXACT)

    first, second = hartley(k1), hartley(k2)
    ones = [spread(index1, first[p::2, :half]) for p in range(2)]
    twos = [spread(index2, second[p::2, : k2 // 2]) for p in range(2)]
    forward = jnp.stack([ones[p // 2] * twos[p % 2] for p in range(4)])
    return (*rounded_halves(forward), *rounded_halves(jnp.swapaxes(forward, 1, 2)))


def dot3(a_top, a_low, b_top, b_low):
    def dot(a, b):
        return jnp.dot(a, b, preferred_element_type=F32)

    return dot(a_top, b_top) + (dot(a_top, b_low) + dot(a_low, b_top))


def lane_of(row, index):
    lanes = lax.broadcasted_iota(jnp.int32, row.shape, 1)
    return jnp.sum(jnp.where(lanes == index, row, 0.0), axis=1, keepdims=True)


def coefficients(parts):
    columns, norms = [], []
    for j, part in enumerate(parts):
        row = jnp.sum(part[...], axis=0)
        norms.append(lane_of(row, j + 2))
        squared = lane_of(row, j + 1)
        columns.append(
            ([lane_of(row, i) / norms[i] for i in range(j + 1)], squared, lax.rsqrt(squared))
        )
    return columns, norms


def orthogonal(raw, vectors, column):
    coeffs, _, scale = column
    for coeff, vector in zip(coeffs, vectors):
        raw = raw - coeff * vector
    return raw * scale


def pieces_of(k1, tones, rows):
    local = rows // (k1 * tones)
    size = k1 // 2 * local
    groups = []
    for a in range(2):
        for b in range(2):
            groups.append(
                [
                    slice(at, at + size)
                    for t in range(tones // 2)
                    for at in [((a * (tones // 2) + t) * k1 + b * (k1 // 2)) * local]
                ]
            )
    return groups


def to_samples(fields, tables, finish):
    top, low = tables[:2]
    sums = [fields[0] + fields[1], fields[2] + fields[3]]
    gaps = [fields[0] - fields[1], fields[2] - fields[3]]
    mixed = [sums[0] + sums[1], sums[0] - sums[1], gaps[0] + gaps[1], gaps[0] - gaps[1]]
    for parity in range(4):
        finish(parity, dot3(top[parity], low[parity], *halves(mixed[parity])))


def to_harmonics(samples, tables):
    top, low = tables[2:]
    parts = [dot3(top[p], low[p], *samples[p]) for p in range(4)]
    even = [parts[0] + parts[1], parts[0] - parts[1]]
    odd = [parts[2] + parts[3], parts[2] - parts[3]]
    return [even[0] + odd[0], even[0] - odd[0], even[1] + odd[1], even[1] - odd[1]]


def taken(value, groups):
    picked = [[value[here, :] for here in group] for group in groups]
    return [p[0] if len(p) == 1 else jnp.concatenate(p, axis=0) for p in picked]


def put(ref, groups, values):
    for group, value in zip(groups, values):
        size = value.shape[0] // len(group)
        for index, here in enumerate(group):
            ref[here, :] = value[index * size : (index + 1) * size, :]


def start_kernel(groups, volts, params, *refs):
    tables, (slope, back) = refs[:4], refs[4:]
    linear, amplitude, sharpness = params[0:1, :], params[1:2, :], params[2:3, :]
    samples = [None] * 4

    def finish(parity, wave):
        size = wave.shape[0]
        bend = jnp.tanh(sharpness * wave)
        here = slice(parity * size, (parity + 1) * size)
        slope[here, :] = linear + amplitude * sharpness * (1.0 - bend * bend)
        samples[parity] = halves(linear * wave + amplitude * bend)

    to_samples(taken(volts, groups), tables, finish)
    put(back, groups, to_harmonics(samples, tables))


def tone_kernel(groups, n_parts, *refs):
    parts, refs = refs[:n_parts], refs[n_parts:]
    raw, basis, refs = refs[0], refs[1 : 1 + n_parts], refs[1 + n_parts :]
    slope, tables, outs = refs[0], refs[1:5], refs[5:]
    fields = taken(raw, groups)
    if n_parts:
        columns, _ = coefficients(parts)
        vectors = [taken(b, groups) for b in basis]
        fields = [
            orthogonal(fields[p], [v[p] for v in vectors], columns[-1]) for p in range(4)
        ]
        put(outs[0], groups, fields)
    samples = [None] * 4

    def finish(parity, wave):
        size = wave.shape[0]
        samples[parity] = halves(slope[parity * size : (parity + 1) * size, :] * wave)

    to_samples(fields, tables, finish)
    put(outs[-1], groups, to_harmonics(samples, tables))


def column_block(width):
    return width // 2 if width % 256 == 0 else width


def columns_call(kernel, name, parts, fields, small, tables, outs):
    rows, width = fields[0].shape
    block = column_block(width)
    whole = pl.BlockSpec((rows, block), lambda i: (0, i))
    once = functools.partial(pl.BlockSpec, pipeline_mode=pl.Buffered(1))
    specs = [once(p.shape, lambda i: (0, 0, 0)) for p in parts]
    specs += [whole for _ in fields]
    specs += [pl.BlockSpec((s.shape[0], block), lambda i: (0, i)) for s in small]
    specs += [once(t.shape, lambda i: (0, 0, 0)) for t in tables]
    return pl.pallas_call(
        kernel,
        name=name,
        grid=(width // block,),
        in_specs=specs,
        out_specs=[whole] * outs,
        out_shape=[jax.ShapeDtypeStruct((rows, width), F32)] * outs,
        compiler_params=pltpu.CompilerParams(vmem_limit_bytes=LIMIT),
        cost_estimate=pl.CostEstimate(
            flops=3 * rows * rows * width, bytes_accessed=16 * rows * width, transcendentals=0
        ),
    )(*parts, *fields, *small, *tables)


def coupled(left, field, right, op_top, op_low, ext_top, ext_low, write):
    width = field.shape[1]
    reach = HALO_B * NB
    for value, at in ((left, 0), (field, reach), (right, reach + width)):
        here = slice(at, at + value.shape[1])
        ext_top[:, here], ext_low[:, here] = halves(value)
    step = 2 * NB if width % (2 * NB) == 0 else NB
    for at in range(0, width, step):
        rows = slice(at, at + step + 2 * reach)
        here = slice(at, at + step)
        write(here, dot3(ext_top[:, rows], ext_low[:, rows], op_top[rows, here], op_low[rows, here]))


def residual_kernel(source, volts, left, right, caps, damps, op_top, op_low, out, ext_top, ext_low):
    def write(here, value):
        scaled = damps[...] * caps[:, here] * volts[:, here]
        out[:, here] = source[:, here] - (scaled + value)

    coupled(left[...], volts[...], right[...], op_top, op_low, ext_top, ext_low, write)


def image_kernel(n_parts, more, *refs):
    parts, refs = refs[:n_parts], refs[n_parts:]
    basis, refs = refs[: n_parts + 1], refs[n_parts + 1 :]
    tones, left, right = refs[0], refs[1][...], refs[2][...]
    lefts, rights = refs[3 : 3 + n_parts], refs[3 + n_parts : 3 + 2 * n_parts]
    refs = refs[3 + 2 * n_parts :]
    caps, damps, op_top, op_low = refs[:4]
    out, stats = refs[4:6]
    refs = refs[6:]
    step = pl.program_id(0)
    if n_parts:
        columns, _ = coefficients(parts)
        left = orthogonal(left, [b[...] for b in lefts], columns[-1])
        right = orthogonal(right, [b[...] for b in rights], columns[-1])
    edges = None
    if more:
        if n_parts:
            refs[0][...] = left
            refs[1][...] = right
            refs = refs[2:]
        edges, refs = refs[:2], refs[2:]
    ext_top, ext_low, sums = refs
    field = basis[-1]

    @pl.when(step == 0)
    def _():
        sums[...] = jnp.zeros_like(sums)

    def tile_sum(value):
        value = jnp.sum(value.reshape(value.shape[0] // 8, 8, value.shape[1]), axis=0)
        total = value[:, :NB]
        for at in range(NB, value.shape[1], NB):
            total = total + value[:, at : at + NB]
        return total

    def write(here, value):
        mine = field[:, here]
        value = value + (tones[:, here] + damps[...] * caps[:, here] * mine)
        out[:, here] = value
        for i in range(n_parts + 1):
            sums[i] += tile_sum(basis[i][:, here] * value)
        sums[n_parts + 1] += tile_sum(value * value)
        sums[n_parts + 2] += tile_sum(mine * mine)

    coupled(left, field[...], right, op_top, op_low, ext_top, ext_low, write)

    if edges:
        take = edges[0].shape[1]
        edges[0][...] = out[:, out.shape[1] - take :]
        edges[1][...] = out[:, :take]

    @pl.when(step == pl.num_programs(0) - 1)
    def _():
        lanes = lax.broadcasted_iota(jnp.int32, (1, NB), 1)
        row = jnp.zeros((1, NB), F32)
        for i in range(n_parts + 3):
            total = jnp.sum(jnp.sum(sums[i], axis=0, keepdims=True), axis=1, keepdims=True)
            row = jnp.where(lanes == i, total, row)
        stats[...] = jnp.broadcast_to(row[None], stats.shape)


def rows_call(kernel, name, parts, fields, caps, damps, operator, outs, stats, scratch):
    rows, width = fields[0].shape
    block = min(rows, ROWS)
    once = functools.partial(pl.BlockSpec, pipeline_mode=pl.Buffered(1))

    def along(shape):
        return pl.BlockSpec((block, shape[1]), lambda i: (i, 0))

    specs = [once(p.shape, lambda i: (0, 0, 0)) for p in parts]
    specs += [along(f.shape) for f in fields]
    small = []
    if caps is not None:
        specs += [once(caps.shape, lambda i: (0, 0)), along(damps.shape)]
        small += [caps, damps]
    specs += [once(o.shape, lambda i: (0, 0)) for o in operator]
    shapes = [jax.ShapeDtypeStruct(o, F32) for o in outs]
    out_specs = [along(o) for o in outs]
    if stats:
        shapes.insert(1, jax.ShapeDtypeStruct((stats, 1, NB), F32))
        out_specs.insert(1, pl.BlockSpec((stats, 1, NB), lambda i: (0, 0, 0)))
    flops = 12 * rows * width * (width + HALO_B * NB) if operator else 16 * rows * width
    return pl.pallas_call(
        kernel,
        name=name,
        grid=(rows // block,),
        in_specs=specs,
        out_specs=out_specs,
        out_shape=shapes,
        scratch_shapes=scratch(block),
        compiler_params=pltpu.CompilerParams(vmem_limit_bytes=LIMIT),
        cost_estimate=pl.CostEstimate(
            flops=flops, bytes_accessed=4 * rows * width * len(fields), transcendentals=0
        ),
    )(*parts, *fields, *small, *operator)


def operator_kernel(band_code, active, coupling, top, low):
    blocks = coupling.shape[0]
    for block in range(blocks):
        cols = slice(block * NB, (block + 1) * NB)
        for row in range(blocks + 2 * HALO_B):
            here = slice(row * NB, (row + 1) * NB)
            offset = row - block
            if 0 <= offset < NOFF:
                band = 0
                for j in range(NOFF):
                    band = band + jnp.where(band_code[j] == offset, j, 0)
                value = jnp.transpose(coupling[block, band]) * active[block, band]
                top[here, cols], low[here, cols] = halves(value)
            else:
                top[here, cols] = jnp.zeros((NB, NB), BF16)
                low[here, cols] = jnp.zeros((NB, NB), BF16)


def band_operator(coupling, band_code, active):
    blocks = coupling.shape[0]
    shape = ((blocks + 2 * HALO_B) * NB, blocks * NB)
    smem = pl.BlockSpec(memory_space=pltpu.SMEM)
    vmem = pl.BlockSpec(memory_space=pltpu.VMEM)
    return pl.pallas_call(
        operator_kernel,
        name="operator",
        in_specs=[smem, smem, vmem],
        out_specs=[vmem, vmem],
        out_shape=[jax.ShapeDtypeStruct(shape, BF16)] * 2,
        compiler_params=pltpu.CompilerParams(vmem_limit_bytes=LIMIT),
        cost_estimate=pl.CostEstimate(flops=1 << 22, bytes_accessed=1 << 22, transcendentals=0),
    )(band_code, active, coupling)


def solve(gram, rhs):
    count = len(rhs)
    lower = [[None] * count for _ in range(count)]
    for i in range(count):
        for j in range(i + 1):
            total = gram[i][j]
            for k in range(j):
                total = total - lower[i][k] * lower[j][k]
            lower[i][j] = jnp.sqrt(total) if i == j else total / lower[j][j]
    forward = []
    for i in range(count):
        total = rhs[i]
        for k in range(i):
            total = total - lower[i][k] * forward[k]
        forward.append(total / lower[i][i])
    backward = [None] * count
    for i in reversed(range(count)):
        total = forward[i]
        for k in range(i + 1, count):
            total = total - lower[k][i] * backward[k]
        backward[i] = total / lower[i][i]
    return backward


def answer_of(parts):
    columns, norms = coefficients(parts)
    hessen = [[None] * M for _ in range(M + 1)]
    for j, (coeffs, squared, scale) in enumerate(columns):
        for i in range(j + 1):
            hessen[i][j] = coeffs[i]
        hessen[j + 1][j] = squared * scale
    gram = [[None] * M for _ in range(M)]
    for j in range(M):
        for i in range(j):
            total = norms[0] * hessen[0][i] * hessen[0][j]
            for k in range(1, i + 2):
                total = total + norms[k] * hessen[k][i] * hessen[k][j]
            gram[j][i] = total
        gram[j][j] = columns[j][1]
    answer = solve(gram, [norms[0] * hessen[0][j] for j in range(M)])
    fitted = []
    for i in range(M):
        first = max(i - 1, 0)
        total = hessen[i][first] * answer[first]
        for j in range(first + 1, M - 1):
            total = total + hessen[i][j] * answer[j]
        fitted.append(total)
    return answer, fitted


def update_kernel(*refs):
    parts, basis, (volts, out) = refs[:M], refs[M : 2 * M], refs[2 * M :]
    answer, _ = answer_of(parts)
    total = answer[0] * basis[0][...]
    for j in range(1, M):
        total = total + answer[j] * basis[j][...]
    out[...] = volts[...] + total


def remaining_kernel(*refs):
    parts, basis, (image, out) = refs[:M], refs[M : 2 * M], refs[2 * M :]
    answer, fitted = answer_of(parts)
    total = basis[0][...] - fitted[0] * basis[0][...]
    for i in range(1, M):
        total = total - fitted[i] * basis[i][...]
    out[...] = total - answer[M - 1] * image[...]


def make(nodes, tones):
    chain = Chain(nodes, tones)
    count = nodes * tones

    def per_device(voltages, source, coupling, band_code, active, cap, damp, kind, type_params):
        node, tone = lax.axis_index("node"), lax.axis_index("tone")
        place = {"tone": tone, "group": node // 2, "core": node % 2}
        place["turn"] = turned(tones, place, tone)
        shape = voltages.shape
        k1, k2 = shape[0], shape[1] * tones

        volts = gather_tones(chain, voltages, place)
        rows, width = volts.shape
        local = rows // tones

        onehot = (kind[None, :] == jnp.arange(NTYPES, dtype=jnp.int32)[:, None]).astype(F32)
        per_node = jnp.dot(type_params, onehot, precision=EXACT)
        per_node = jnp.concatenate(
            [per_node, cap[None, :], jnp.zeros((4, cap.shape[0]), F32)], axis=0
        )
        per_node = chunk_of(chain, per_node, place, 1)
        caps = per_node[3:4]
        damps = jnp.zeros((tones, local, 1), F32)
        for s in range(tones):
            piece = lax.ppermute(damp, AXES, chain.shift(s)) if s else damp
            piece = piece.reshape(1, local, 1)
            damps = lax.dynamic_update_slice_in_dim(damps, piece, (tone - s) % tones, 0)
        damps = damps.reshape(rows, 1)

        def ext_scratch(nodes):
            ext = nodes + 2 * HALO_B * NB
            return lambda block: [pltpu.VMEM((block, ext), BF16)] * 2

        volts_here = voltages.reshape(local, shape[2])
        left, right = halos(*edges_of(volts_here), chain.node_up, chain.node_down)
        (driven,) = rows_call(
            residual_kernel,
            "driven",
            [],
            [source.reshape(local, shape[2]), volts_here, left, right],
            cap[None, :],
            damp.reshape(local, 1),
            band_operator(coupling, band_code, active.astype(F32)),
            [(local, shape[2])],
            0,
            ext_scratch(shape[2]),
        )
        driven, volts, coupling = lax.optimization_barrier((driven, volts, coupling))
        driven = gather_tones(chain, driven.reshape(shape), place)

        mine = chunk_of(chain, coupling, place, 0)
        mine_active = chunk_of(chain, active.astype(F32), place, 0)
        operator = band_operator(mine, band_code, mine_active)
        tables = two_tone_tables(k1, k2, tones)
        groups = pieces_of(k1, tones, rows)

        slope, back = columns_call(
            functools.partial(start_kernel, groups), "start", [], [volts], [per_node], tables, 2
        )
        start = driven - back

        left, right = halos(*edges_of(start), chain.up, chain.down)
        basis, lefts, rights, parts = [], [], [], []
        image = start
        edge, reach = (rows, min(width, HALO_B * NB)), (rows, HALO_B * NB)
        for column in range(M):
            made = columns_call(
                functools.partial(tone_kernel, groups, column),
                f"tone{column}",
                parts,
                [image, *basis, slope],
                [],
                tables,
                2 if column else 1,
            )
            new, toned = made if column else (start, made[0])
            more = column + 1 < M
            made = rows_call(
                functools.partial(image_kernel, column, more),
                f"image{column}",
                parts,
                [*basis, new, toned, left, right, *lefts, *rights],
                caps,
                damps,
                operator,
                [(rows, width)] + ([reach, reach] if more and column else []) + [edge, edge] * more,
                count,
                lambda block, n=column: ext_scratch(width)(block)
                + [pltpu.VMEM((n + 3, 8, NB), F32)],
            )
            image, stats = made[:2]
            basis.append(new)
            part = lax.all_to_all(stats, AXES, 0, 0, tiled=True)
            if more:
                lefts.append(made[2] if column else left)
                rights.append(made[3] if column else right)
                last, first, part = lax.optimization_barrier((*made[-2:], part))
                left, right = halos(last, first, chain.up, chain.down)
            parts = parts + [part]

        def final(kernel, name, last):
            return rows_call(
                kernel, name, parts, [*basis, last], None, None, [], [(rows, width)], 0, lambda block: []
            )[0]

        new_volts = scatter_tones(chain, final(update_kernel, "update", volts), place, shape)
        remaining = scatter_tones(chain, final(remaining_kernel, "remaining", image), place, shape)
        return new_volts, remaining

    return per_device


def solution(mesh):
    placed = (
        P(None, "tone", "node"),
        P(None, "tone", "node"),
        P("node", None, None, None),
        P(),
        P("node", None),
        P("node"),
        P(None, "tone"),
        P("node"),
        P(),
    )
    return jax.shard_map(
        make(mesh.shape["node"], mesh.shape["tone"]),
        mesh=mesh,
        in_specs=placed,
        out_specs=(P(None, "tone", "node"), P(None, "tone", "node")),
        check_vma=False,
    )
```

```python
import functools
import math

import jax
import jax.numpy as jnp
from jax import lax
from jax.experimental import pallas as pl
from jax.experimental.pallas import tpu as pltpu
from jax.sharding import PartitionSpec as P

NB = 128
HALO_B = 3
NOFF = 7
M = 4
NTYPES = 4
AXES = ("node", "tone")
EXACT = lax.Precision.HIGHEST
F32 = jnp.float32
BF16 = jnp.bfloat16
LIMIT = 16 * 1024 * 1024
ROWS = 128


class Chain:
    def __init__(self, nodes, tones):
        self.nodes, self.tones = nodes, tones
        self.at = [0] * (nodes * tones)
        for i in range(nodes):
            for t in range(tones):
                place = (i // 2) * 2 * tones + 2 * self.turn(i, t) + i % 2
                self.at[place] = i * tones + t

    def turn(self, i, t):
        return t if (i // 2) % 2 == 0 else self.tones - 1 - t

    def device(self, group, core, turn):
        return self.at[group * 2 * self.tones + 2 * turn + core]

    def up(self, hop):
        return [(self.at[p], self.at[p + hop]) for p in range(len(self.at) - hop)]

    def down(self, hop):
        return [(b, a) for a, b in self.up(hop)]

    def node_up(self, hop):
        tones = self.tones
        return [
            (i * tones + t, (i + hop) * tones + t)
            for i in range(self.nodes - hop)
            for t in range(tones)
        ]

    def node_down(self, hop):
        return [(b, a) for a, b in self.node_up(hop)]

    def swap(self):
        tones = self.tones
        return [(i * tones + t, (i ^ 1) * tones + t) for i in range(self.nodes) for t in range(tones)]

    def shift(self, s):
        tones = self.tones
        return [
            (i * tones + t, i * tones + (t + s) % tones)
            for i in range(self.nodes)
            for t in range(tones)
        ]

    def first(self):
        pairs = []
        for g in range(self.nodes // 2):
            for a, b in (((0, 0), (1, 0)), ((0, 1), (0, 0)), ((1, 0), (1, 1)), ((1, 1), (0, 1))):
                pairs.append((self.device(g, *a), self.device(g, *b)))
        return pairs

    def second(self):
        pairs = []
        for g in range(self.nodes // 2):
            for a, b in (((0, 1), (1, 0)), ((1, 0), (0, 1))):
                pairs.append((self.device(g, *a), self.device(g, *b)))
        return pairs


def flipped(pairs):
    return [(b, a) for a, b in pairs]


def turned(tones, place, index):
    return jnp.where((place["group"] % 2) == 0, index, tones - 1 - index)


def parity_chunks(value, tones, parity, axis):
    width = value.shape[axis] // tones
    parts = [
        lax.dynamic_slice_in_dim(value, (2 * h + parity) * width, width, axis)
        for h in range(tones // 2)
    ]
    return parts[0] if len(parts) == 1 else jnp.concatenate(parts, axis=axis)


def core_swap(chain, value, core, axis):
    keep = parity_chunks(value, chain.tones, core, axis)
    give = parity_chunks(value, chain.tones, 1 - core, axis)
    got = lax.ppermute(give, AXES, chain.swap())
    return jnp.where(core == 0, keep, got), jnp.where(core == 0, got, keep)


def chunk_of(chain, value, place, axis):
    low, high = core_swap(chain, value, place["core"], axis)
    half = chain.tones // 2
    both = jnp.where(place["turn"] < half, low, high)
    width = value.shape[axis] // chain.tones
    return lax.dynamic_slice_in_dim(both, place["turn"] % half * width, width, axis)


def gather_tones(chain, field, place):
    tones, tone, core, turn = chain.tones, place["tone"], place["core"], place["turn"]
    width = field.shape[2] // tones
    rows = field.shape[0] * field.shape[1]
    field = field.reshape(rows, field.shape[2])
    if tones == 2:
        one = lax.dynamic_slice_in_dim(field, (1 - turn) * width, width, 1)
        two = lax.dynamic_slice_in_dim(field, turn * width, width, 1)
        got_one = lax.ppermute(one, AXES, chain.first())
        got_two = lax.ppermute(two, AXES, chain.second())
        same = jnp.where(core == turn, two, got_one)
        other = jnp.where(core == turn, got_one, got_two)
        return jnp.concatenate(
            [jnp.where(tone == 0, same, other), jnp.where(tone == 0, other, same)], axis=0
        )
    low, high = core_swap(chain, field, core, 1)
    chunks = jnp.concatenate([low, high], axis=1)
    out = jnp.zeros((tones * rows, width), field.dtype)
    for s in range(tones):
        target = turned(tones, place, (tone + s) % tones)
        piece = lax.dynamic_slice_in_dim(chunks, target * width, width, 1)
        if s:
            piece = lax.ppermute(piece, AXES, chain.shift(s))
        out = lax.dynamic_update_slice_in_dim(out, piece, (tone - s) % tones * rows, 0)
    return out


def scatter_tones(chain, field, place, shape):
    tones, tone, core, turn = chain.tones, place["tone"], place["core"], place["turn"]
    width = field.shape[1]
    rows = field.shape[0] // tones
    if tones == 2:
        same = lax.dynamic_slice_in_dim(field, tone * rows, rows, 0)
        other = lax.dynamic_slice_in_dim(field, (1 - tone) * rows, rows, 0)
        one = jnp.where(core == turn, other, same)
        got_one = lax.ppermute(one, AXES, flipped(chain.first()))
        got_two = lax.ppermute(other, AXES, flipped(chain.second()))
        at_turn = jnp.where(core == turn, same, got_two)
        return jnp.concatenate(
            [jnp.where(turn == 0, at_turn, got_one), jnp.where(turn == 0, got_one, at_turn)], axis=1
        ).reshape(shape)
    chunks = jnp.zeros((rows, tones * width), field.dtype)
    for s in range(tones):
        piece = lax.dynamic_slice_in_dim(field, (tone + s) % tones * rows, rows, 0)
        if s:
            piece = lax.ppermute(piece, AXES, chain.shift(s))
        slot = turned(tones, place, (tone - s) % tones)
        chunks = lax.dynamic_update_slice_in_dim(chunks, piece, slot * width, 1)
    half = tones // 2 * width
    low, high = chunks[:, :half], chunks[:, half:]
    keep = jnp.where(core == 0, low, high)
    give = jnp.where(core == 0, high, low)
    got = lax.ppermute(give, AXES, chain.swap())
    even, odd = jnp.where(core == 0, keep, got), jnp.where(core == 0, got, keep)
    parts = []
    for h in range(tones // 2):
        parts += [even[:, h * width : (h + 1) * width], odd[:, h * width : (h + 1) * width]]
    return jnp.concatenate(parts, axis=1).reshape(shape)


def edges_of(field):
    take = min(field.shape[1], HALO_B * NB)
    return field[:, field.shape[1] - take :], field[:, :take]


def halos(last, first, up, down):
    width = last.shape[1]
    reach = HALO_B * NB
    left, right = [], []
    hop, have = 1, 0
    while have < reach:
        take = min(width, reach - have)
        left.insert(0, lax.ppermute(last[:, width - take :], AXES, up(hop)))
        right.append(lax.ppermute(first[:, :take], AXES, down(hop)))
        have, hop = have + take, hop + 1
    if len(left) == 1:
        return left[0], right[0]
    return jnp.concatenate(left, axis=1), jnp.concatenate(right, axis=1)


def hartley(count):
    grid = jnp.arange(count, dtype=jnp.int32)
    phase = grid[:, None] * grid[None, :] % count
    angle = phase.astype(F32) * (2.0 * math.pi / count)
    return (jnp.cos(angle) + jnp.sin(angle)) / math.sqrt(count)


def halves(value):
    top = value.astype(BF16)
    return top, (value - top.astype(F32)).astype(BF16)


def rounded_halves(value):
    top = lax.reduce_precision(value, exponent_bits=8, mantissa_bits=7)
    return top.astype(BF16), (value - top).astype(BF16)


def two_tone_tables(k1, k2, tones):
    local, half = k2 // tones, k1 // 2
    rows = jnp.arange(half * k2 // 2, dtype=jnp.int32)
    index1 = rows // local % half
    index2 = rows // (local * half) * local + rows % local

    def spread(index, table):
        pick = (index[:, None] == jnp.arange(table.shape[0], dtype=jnp.int32)[None, :]).astype(F32)
        left = jnp.dot(pick, table, precision=EXACT)
        return lax.dot_general(left, pick, (((1,), (1,)), ((), ())), precision=EXACT)

    first, second = hartley(k1), hartley(k2)
    ones = [spread(index1, first[p::2, :half]) for p in range(2)]
    twos = [spread(index2, second[p::2, : k2 // 2]) for p in range(2)]
    forward = jnp.stack([ones[p // 2] * twos[p % 2] for p in range(4)])
    return (*rounded_halves(forward), *rounded_halves(jnp.swapaxes(forward, 1, 2)))


def dot3(a_top, a_low, b_top, b_low):
    def dot(a, b):
        return jnp.dot(a, b, preferred_element_type=F32)

    return dot(a_top, b_top) + (dot(a_top, b_low) + dot(a_low, b_top))


def lane_of(row, index):
    lanes = lax.broadcasted_iota(jnp.int32, row.shape, 1)
    return jnp.sum(jnp.where(lanes == index, row, 0.0), axis=1, keepdims=True)


def coefficients(parts):
    columns, norms = [], []
    for j, part in enumerate(parts):
        row = jnp.sum(part[...], axis=0)
        norms.append(lane_of(row, j + 2))
        squared = lane_of(row, j + 1)
        columns.append(
            ([lane_of(row, i) / norms[i] for i in range(j + 1)], squared, lax.rsqrt(squared))
        )
    return columns, norms


def orthogonal(raw, vectors, column):
    coeffs, _, scale = column
    for coeff, vector in zip(coeffs, vectors):
        raw = raw - coeff * vector
    return raw * scale


def pieces_of(k1, tones, rows):
    local = rows // (k1 * tones)
    size = k1 // 2 * local
    groups = []
    for a in range(2):
        for b in range(2):
            groups.append(
                [
                    slice(at, at + size)
                    for t in range(tones // 2)
                    for at in [((a * (tones // 2) + t) * k1 + b * (k1 // 2)) * local]
                ]
            )
    return groups


def to_samples(fields, tables, finish):
    top, low = tables[:2]
    sums = [fields[0] + fields[1], fields[2] + fields[3]]
    gaps = [fields[0] - fields[1], fields[2] - fields[3]]
    mixed = [sums[0] + sums[1], sums[0] - sums[1], gaps[0] + gaps[1], gaps[0] - gaps[1]]
    for parity in range(4):
        finish(parity, dot3(top[parity], low[parity], *halves(mixed[parity])))


def to_harmonics(samples, tables):
    top, low = tables[2:]
    parts = [dot3(top[p], low[p], *samples[p]) for p in range(4)]
    even = [parts[0] + parts[1], parts[0] - parts[1]]
    odd = [parts[2] + parts[3], parts[2] - parts[3]]
    return [even[0] + odd[0], even[0] - odd[0], even[1] + odd[1], even[1] - odd[1]]


def taken(value, groups):
    picked = [[value[here, :] for here in group] for group in groups]
    return [p[0] if len(p) == 1 else jnp.concatenate(p, axis=0) for p in picked]


def put(ref, groups, values):
    for group, value in zip(groups, values):
        size = value.shape[0] // len(group)
        for index, here in enumerate(group):
            ref[here, :] = value[index * size : (index + 1) * size, :]


def start_kernel(groups, volts, params, *refs):
    tables, (slope, back) = refs[:4], refs[4:]
    linear, amplitude, sharpness = params[0:1, :], params[1:2, :], params[2:3, :]
    samples = [None] * 4

    def finish(parity, wave):
        size = wave.shape[0]
        bend = jnp.tanh(sharpness * wave)
        here = slice(parity * size, (parity + 1) * size)
        slope[here, :] = linear + amplitude * sharpness * (1.0 - bend * bend)
        samples[parity] = halves(linear * wave + amplitude * bend)

    to_samples(taken(volts, groups), tables, finish)
    put(back, groups, to_harmonics(samples, tables))


def tone_kernel(groups, n_parts, *refs):
    parts, refs = refs[:n_parts], refs[n_parts:]
    raw, basis, refs = refs[0], refs[1 : 1 + n_parts], refs[1 + n_parts :]
    slope, tables, outs = refs[0], refs[1:5], refs[5:]
    fields = taken(raw, groups)
    if n_parts:
        columns, _ = coefficients(parts)
        vectors = [taken(b, groups) for b in basis]
        fields = [
            orthogonal(fields[p], [v[p] for v in vectors], columns[-1]) for p in range(4)
        ]
        put(outs[0], groups, fields)
    samples = [None] * 4

    def finish(parity, wave):
        size = wave.shape[0]
        samples[parity] = halves(slope[parity * size : (parity + 1) * size, :] * wave)

    to_samples(fields, tables, finish)
    put(outs[-1], groups, to_harmonics(samples, tables))


def column_block(width):
    return width // 2 if width % 256 == 0 else width


def columns_call(kernel, parts, fields, small, tables, outs):
    rows, width = fields[0].shape
    block = column_block(width)
    whole = pl.BlockSpec((rows, block), lambda i: (0, i))
    once = functools.partial(pl.BlockSpec, pipeline_mode=pl.Buffered(1))
    specs = [once(p.shape, lambda i: (0, 0, 0)) for p in parts]
    specs += [whole for _ in fields]
    specs += [pl.BlockSpec((s.shape[0], block), lambda i: (0, i)) for s in small]
    specs += [once(t.shape, lambda i: (0, 0, 0)) for t in tables]
    return pl.pallas_call(
        kernel,
        grid=(width // block,),
        in_specs=specs,
        out_specs=[whole] * outs,
        out_shape=[jax.ShapeDtypeStruct((rows, width), F32)] * outs,
        compiler_params=pltpu.CompilerParams(vmem_limit_bytes=LIMIT),
        cost_estimate=pl.CostEstimate(
            flops=3 * rows * rows * width, bytes_accessed=16 * rows * width, transcendentals=0
        ),
    )(*parts, *fields, *small, *tables)


def coupled(left, field, right, op_top, op_low, ext_top, ext_low, write):
    width = field.shape[1]
    reach = HALO_B * NB
    for value, at in ((left, 0), (field, reach), (right, reach + width)):
        here = slice(at, at + value.shape[1])
        ext_top[:, here], ext_low[:, here] = halves(value)
    step = 2 * NB if width % (2 * NB) == 0 else NB
    for at in range(0, width, step):
        rows = slice(at, at + step + 2 * reach)
        here = slice(at, at + step)
        write(here, dot3(ext_top[:, rows], ext_low[:, rows], op_top[rows, here], op_low[rows, here]))


def residual_kernel(source, volts, left, right, caps, damps, op_top, op_low, out, ext_top, ext_low):
    def write(here, value):
        scaled = damps[...] * caps[:, here] * volts[:, here]
        out[:, here] = source[:, here] - (scaled + value)

    coupled(left[...], volts[...], right[...], op_top, op_low, ext_top, ext_low, write)


def image_kernel(n_parts, more, *refs):
    parts, refs = refs[:n_parts], refs[n_parts:]
    basis, refs = refs[: n_parts + 1], refs[n_parts + 1 :]
    tones, left, right = refs[0], refs[1][...], refs[2][...]
    lefts, rights = refs[3 : 3 + n_parts], refs[3 + n_parts : 3 + 2 * n_parts]
    refs = refs[3 + 2 * n_parts :]
    caps, damps, op_top, op_low = refs[:4]
    out, stats = refs[4:6]
    refs = refs[6:]
    step = pl.program_id(0)
    if n_parts:
        columns, _ = coefficients(parts)
        left = orthogonal(left, [b[...] for b in lefts], columns[-1])
        right = orthogonal(right, [b[...] for b in rights], columns[-1])
    edges = None
    if more:
        if n_parts:
            refs[0][...] = left
            refs[1][...] = right
            refs = refs[2:]
        edges, refs = refs[:2], refs[2:]
    ext_top, ext_low, sums = refs
    field = basis[-1]

    @pl.when(step == 0)
    def _():
        sums[...] = jnp.zeros_like(sums)

    def tile_sum(value):
        value = jnp.sum(value.reshape(value.shape[0] // 8, 8, value.shape[1]), axis=0)
        total = value[:, :NB]
        for at in range(NB, value.shape[1], NB):
            total = total + value[:, at : at + NB]
        return total

    def write(here, value):
        mine = field[:, here]
        value = value + (tones[:, here] + damps[...] * caps[:, here] * mine)
        out[:, here] = value
        for i in range(n_parts + 1):
            sums[i] += tile_sum(basis[i][:, here] * value)
        sums[n_parts + 1] += tile_sum(value * value)
        sums[n_parts + 2] += tile_sum(mine * mine)

    coupled(left, field[...], right, op_top, op_low, ext_top, ext_low, write)

    if edges:
        take = edges[0].shape[1]
        edges[0][...] = out[:, out.shape[1] - take :]
        edges[1][...] = out[:, :take]

    @pl.when(step == pl.num_programs(0) - 1)
    def _():
        lanes = lax.broadcasted_iota(jnp.int32, (1, NB), 1)
        row = jnp.zeros((1, NB), F32)
        for i in range(n_parts + 3):
            total = jnp.sum(jnp.sum(sums[i], axis=0, keepdims=True), axis=1, keepdims=True)
            row = jnp.where(lanes == i, total, row)
        stats[...] = jnp.broadcast_to(row[None], stats.shape)


def rows_call(kernel, parts, fields, caps, damps, operator, outs, stats, scratch):
    rows, width = fields[0].shape
    block = min(rows, ROWS)
    once = functools.partial(pl.BlockSpec, pipeline_mode=pl.Buffered(1))

    def along(shape):
        return pl.BlockSpec((block, shape[1]), lambda i: (i, 0))

    specs = [once(p.shape, lambda i: (0, 0, 0)) for p in parts]
    specs += [along(f.shape) for f in fields]
    small = []
    if caps is not None:
        specs += [once(caps.shape, lambda i: (0, 0)), along(damps.shape)]
        small += [caps, damps]
    specs += [once(o.shape, lambda i: (0, 0)) for o in operator]
    shapes = [jax.ShapeDtypeStruct(o, F32) for o in outs]
    out_specs = [along(o) for o in outs]
    if stats:
        shapes.insert(1, jax.ShapeDtypeStruct((stats, 1, NB), F32))
        out_specs.insert(1, pl.BlockSpec((stats, 1, NB), lambda i: (0, 0, 0)))
    flops = 12 * rows * width * (width + HALO_B * NB) if operator else 16 * rows * width
    return pl.pallas_call(
        kernel,
        grid=(rows // block,),
        in_specs=specs,
        out_specs=out_specs,
        out_shape=shapes,
        scratch_shapes=scratch(block),
        compiler_params=pltpu.CompilerParams(vmem_limit_bytes=LIMIT),
        cost_estimate=pl.CostEstimate(
            flops=flops, bytes_accessed=4 * rows * width * len(fields), transcendentals=0
        ),
    )(*parts, *fields, *small, *operator)


def operator_kernel(band_code, active, coupling, top, low):
    blocks = coupling.shape[0]
    for block in range(blocks):
        cols = slice(block * NB, (block + 1) * NB)
        for row in range(blocks + 2 * HALO_B):
            here = slice(row * NB, (row + 1) * NB)
            offset = row - block
            if 0 <= offset < NOFF:
                band = 0
                for j in range(NOFF):
                    band = band + jnp.where(band_code[j] == offset, j, 0)
                value = jnp.transpose(coupling[block, band]) * active[block, band]
                top[here, cols], low[here, cols] = halves(value)
            else:
                top[here, cols] = jnp.zeros((NB, NB), BF16)
                low[here, cols] = jnp.zeros((NB, NB), BF16)


def band_operator(coupling, band_code, active):
    blocks = coupling.shape[0]
    shape = ((blocks + 2 * HALO_B) * NB, blocks * NB)
    smem = pl.BlockSpec(memory_space=pltpu.SMEM)
    vmem = pl.BlockSpec(memory_space=pltpu.VMEM)
    return pl.pallas_call(
        operator_kernel,
        name="operator",
        in_specs=[smem, smem, vmem],
        out_specs=[vmem, vmem],
        out_shape=[jax.ShapeDtypeStruct(shape, BF16)] * 2,
        compiler_params=pltpu.CompilerParams(vmem_limit_bytes=LIMIT),
        cost_estimate=pl.CostEstimate(flops=1 << 22, bytes_accessed=1 << 22, transcendentals=0),
    )(band_code, active, coupling)


def solve(gram, rhs):
    count = len(rhs)
    lower = [[None] * count for _ in range(count)]
    for i in range(count):
        for j in range(i + 1):
            total = gram[i][j]
            for k in range(j):
                total = total - lower[i][k] * lower[j][k]
            lower[i][j] = jnp.sqrt(total) if i == j else total / lower[j][j]
    forward = []
    for i in range(count):
        total = rhs[i]
        for k in range(i):
            total = total - lower[i][k] * forward[k]
        forward.append(total / lower[i][i])
    backward = [None] * count
    for i in reversed(range(count)):
        total = forward[i]
        for k in range(i + 1, count):
            total = total - lower[k][i] * backward[k]
        backward[i] = total / lower[i][i]
    return backward


def answer_of(parts):
    columns, norms = coefficients(parts)
    hessen = [[None] * M for _ in range(M + 1)]
    for j, (coeffs, squared, scale) in enumerate(columns):
        for i in range(j + 1):
            hessen[i][j] = coeffs[i]
        hessen[j + 1][j] = squared * scale
    gram = [[None] * M for _ in range(M)]
    for j in range(M):
        for i in range(j):
            total = norms[0] * hessen[0][i] * hessen[0][j]
            for k in range(1, i + 2):
                total = total + norms[k] * hessen[k][i] * hessen[k][j]
            gram[j][i] = total
        gram[j][j] = columns[j][1]
    answer = solve(gram, [norms[0] * hessen[0][j] for j in range(M)])
    fitted = []
    for i in range(M):
        first = max(i - 1, 0)
        total = hessen[i][first] * answer[first]
        for j in range(first + 1, M - 1):
            total = total + hessen[i][j] * answer[j]
        fitted.append(total)
    return answer, fitted


def final_kernel(*refs):
    parts, basis, (volts, image, updated, remaining) = refs[:M], refs[M : 2 * M], refs[2 * M :]
    answer, fitted = answer_of(parts)
    total = answer[0] * basis[0][...]
    rest = basis[0][...] - fitted[0] * basis[0][...]
    for j in range(1, M):
        vector = basis[j][...]
        total = total + answer[j] * vector
        rest = rest - fitted[j] * vector
    updated[...] = volts[...] + total
    remaining[...] = rest - answer[M - 1] * image[...]


def make(nodes, tones):
    chain = Chain(nodes, tones)
    count = nodes * tones

    def per_device(voltages, source, coupling, band_code, active, cap, damp, kind, type_params):
        node, tone = lax.axis_index("node"), lax.axis_index("tone")
        place = {"tone": tone, "group": node // 2, "core": node % 2}
        place["turn"] = turned(tones, place, tone)
        shape = voltages.shape
        k1, k2 = shape[0], shape[1] * tones

        volts = gather_tones(chain, voltages, place)
        rows, width = volts.shape
        local = rows // tones

        onehot = (kind[None, :] == jnp.arange(NTYPES, dtype=jnp.int32)[:, None]).astype(F32)
        per_node = jnp.dot(type_params, onehot, precision=EXACT)
        per_node = jnp.concatenate(
            [per_node, cap[None, :], jnp.zeros((4, cap.shape[0]), F32)], axis=0
        )
        per_node = chunk_of(chain, per_node, place, 1)
        damps = jnp.zeros((tones, local, 1), F32)
        for s in range(tones):
            piece = lax.ppermute(damp, AXES, chain.shift(s)) if s else damp
            piece = piece.reshape(1, local, 1)
            damps = lax.dynamic_update_slice_in_dim(damps, piece, (tone - s) % tones, 0)
        damps = damps.reshape(rows, 1)

        def ext_scratch(nodes):
            ext = nodes + 2 * HALO_B * NB
            return lambda block: [pltpu.VMEM((block, ext), BF16)] * 2

        volts_here = voltages.reshape(local, shape[2])
        left, right = halos(*edges_of(volts_here), chain.node_up, chain.node_down)
        (driven,) = rows_call(
            residual_kernel,
            [],
            [source.reshape(local, shape[2]), volts_here, left, right],
            cap[None, :],
            damp.reshape(local, 1),
            band_operator(coupling, band_code, active.astype(F32)),
            [(local, shape[2])],
            0,
            ext_scratch(shape[2]),
        )
        mine = chunk_of(chain, coupling, place, 0)
        mine_active = chunk_of(chain, active.astype(F32), place, 0)
        driven, damps, mine, mine_active, per_node = lax.optimization_barrier(
            (driven, damps, mine, mine_active, per_node)
        )
        caps = per_node[3:4]
        driven = gather_tones(chain, driven.reshape(shape), place)

        operator = band_operator(mine, band_code, mine_active)
        tables = two_tone_tables(k1, k2, tones)
        groups = pieces_of(k1, tones, rows)

        slope, back = columns_call(
            functools.partial(start_kernel, groups), [], [volts], [per_node], tables, 2
        )
        start = driven - back

        left, right = halos(*edges_of(start), chain.up, chain.down)
        basis, lefts, rights, parts = [], [], [], []
        image = start
        edge, reach = (rows, min(width, HALO_B * NB)), (rows, HALO_B * NB)
        for column in range(M):
            made = columns_call(
                functools.partial(tone_kernel, groups, column),
                parts,
                [image, *basis, slope],
                [],
                tables,
                2 if column else 1,
            )
            new, toned = made if column else (start, made[0])
            more = column + 1 < M
            made = rows_call(
                functools.partial(image_kernel, column, more),
                parts,
                [*basis, new, toned, left, right, *lefts, *rights],
                caps,
                damps,
                operator,
                [(rows, width)] + ([reach, reach] if more and column else []) + [edge, edge] * more,
                count,
                lambda block, n=column: ext_scratch(width)(block)
                + [pltpu.VMEM((n + 3, 8, NB), F32)],
            )
            image, stats = made[:2]
            basis.append(new)
            if more:
                lefts.append(made[2] if column else left)
                rights.append(made[3] if column else right)
                left, right = halos(*made[-2:], chain.up, chain.down)
            part = lax.all_to_all(stats, AXES, 0, 0, tiled=True)
            parts = parts + [part]

        new_volts, remaining = rows_call(
            final_kernel,
            parts,
            [*basis, volts, image],
            None,
            None,
            [],
            [(rows, width)] * 2,
            0,
            lambda block: [],
        )
        new_volts = scatter_tones(chain, new_volts, place, shape)
        remaining = scatter_tones(chain, remaining, place, shape)
        return new_volts, remaining

    return per_device


def solution(mesh):
    placed = (
        P(None, "tone", "node"),
        P(None, "tone", "node"),
        P("node", None, None, None),
        P(),
        P("node", None),
        P("node"),
        P(None, "tone"),
        P("node"),
        P(),
    )
    body = make(mesh.shape["node"], mesh.shape["tone"])

    return jax.shard_map(
        body,
        mesh=mesh,
        in_specs=placed,
        out_specs=(P(None, "tone", "node"), P(None, "tone", "node")),
        check_vma=False,
    )
```

```python
import functools
import math

import jax
import jax.numpy as jnp
from jax import lax
from jax.experimental import pallas as pl
from jax.experimental.pallas import tpu as pltpu
from jax.sharding import PartitionSpec as P

NB = 128
HALO_B = 3
NOFF = 7
M = 4
NTYPES = 4
AXES = ("node", "tone")
EXACT = lax.Precision.HIGHEST
F32 = jnp.float32
BF16 = jnp.bfloat16
LIMIT = 16 * 1024 * 1024
LIMIT_START = 60 * 1024 * 1024
LIMIT_END = 60 * 1024 * 1024
ROWS = 256


class Chain:
    def __init__(self, nodes, tones):
        self.nodes, self.tones = nodes, tones
        self.at = [0] * (nodes * tones)
        for i in range(nodes):
            for t in range(tones):
                place = (i // 2) * 2 * tones + 2 * self.turn(i, t) + i % 2
                self.at[place] = i * tones + t

    def turn(self, i, t):
        return t if (i // 2) % 2 == 0 else self.tones - 1 - t

    def device(self, group, core, turn):
        return self.at[group * 2 * self.tones + 2 * turn + core]

    def up(self, hop):
        return [(self.at[p], self.at[p + hop]) for p in range(len(self.at) - hop)]

    def down(self, hop):
        return [(b, a) for a, b in self.up(hop)]

    def node_up(self, hop):
        tones = self.tones
        return [
            (i * tones + t, (i + hop) * tones + t)
            for i in range(self.nodes - hop)
            for t in range(tones)
        ]

    def node_down(self, hop):
        return [(b, a) for a, b in self.node_up(hop)]

    def swap(self):
        tones = self.tones
        return [(i * tones + t, (i ^ 1) * tones + t) for i in range(self.nodes) for t in range(tones)]

    def shift(self, s):
        tones = self.tones
        return [
            (i * tones + t, i * tones + (t + s) % tones)
            for i in range(self.nodes)
            for t in range(tones)
        ]

    def first(self):
        pairs = []
        for g in range(self.nodes // 2):
            for a, b in (((0, 0), (1, 0)), ((0, 1), (0, 0)), ((1, 0), (1, 1)), ((1, 1), (0, 1))):
                pairs.append((self.device(g, *a), self.device(g, *b)))
        return pairs

    def second(self):
        pairs = []
        for g in range(self.nodes // 2):
            for a, b in (((0, 1), (1, 0)), ((1, 0), (0, 1))):
                pairs.append((self.device(g, *a), self.device(g, *b)))
        return pairs


def flipped(pairs):
    return [(b, a) for a, b in pairs]


def turned(tones, place, index):
    return jnp.where((place["group"] % 2) == 0, index, tones - 1 - index)


def parity_chunks(value, tones, parity, axis):
    width = value.shape[axis] // tones
    parts = [
        lax.dynamic_slice_in_dim(value, (2 * h + parity) * width, width, axis)
        for h in range(tones // 2)
    ]
    return parts[0] if len(parts) == 1 else jnp.concatenate(parts, axis=axis)


def core_swap(chain, value, core, axis):
    keep = parity_chunks(value, chain.tones, core, axis)
    give = parity_chunks(value, chain.tones, 1 - core, axis)
    got = lax.ppermute(give, AXES, chain.swap())
    return jnp.where(core == 0, keep, got), jnp.where(core == 0, got, keep)


def chunk_of(chain, value, place, axis):
    low, high = core_swap(chain, value, place["core"], axis)
    half = chain.tones // 2
    both = jnp.where(place["turn"] < half, low, high)
    width = value.shape[axis] // chain.tones
    return lax.dynamic_slice_in_dim(both, place["turn"] % half * width, width, axis)


def gather_tones(chain, field, place):
    tones, tone, core, turn = chain.tones, place["tone"], place["core"], place["turn"]
    width = field.shape[2] // tones
    rows = field.shape[0] * field.shape[1]
    field = field.reshape(rows, field.shape[2])
    if tones == 2:
        one = lax.dynamic_slice_in_dim(field, (1 - turn) * width, width, 1)
        two = lax.dynamic_slice_in_dim(field, turn * width, width, 1)
        got_one = lax.ppermute(one, AXES, chain.first())
        got_two = lax.ppermute(two, AXES, chain.second())
        same = jnp.where(core == turn, two, got_one)
        other = jnp.where(core == turn, got_one, got_two)
        return jnp.concatenate(
            [jnp.where(tone == 0, same, other), jnp.where(tone == 0, other, same)], axis=0
        )
    low, high = core_swap(chain, field, core, 1)
    chunks = jnp.concatenate([low, high], axis=1)
    out = jnp.zeros((tones * rows, width), field.dtype)
    for s in range(tones):
        target = turned(tones, place, (tone + s) % tones)
        piece = lax.dynamic_slice_in_dim(chunks, target * width, width, 1)
        if s:
            piece = lax.ppermute(piece, AXES, chain.shift(s))
        out = lax.dynamic_update_slice_in_dim(out, piece, (tone - s) % tones * rows, 0)
    return out


def scatter_tones(chain, field, place, shape):
    tones, tone, core, turn = chain.tones, place["tone"], place["core"], place["turn"]
    width = field.shape[1]
    rows = field.shape[0] // tones
    if tones == 2:
        same = lax.dynamic_slice_in_dim(field, tone * rows, rows, 0)
        other = lax.dynamic_slice_in_dim(field, (1 - tone) * rows, rows, 0)
        one = jnp.where(core == turn, other, same)
        got_one = lax.ppermute(one, AXES, flipped(chain.first()))
        got_two = lax.ppermute(other, AXES, flipped(chain.second()))
        at_turn = jnp.where(core == turn, same, got_two)
        return jnp.concatenate(
            [jnp.where(turn == 0, at_turn, got_one), jnp.where(turn == 0, got_one, at_turn)], axis=1
        ).reshape(shape)
    chunks = jnp.zeros((rows, tones * width), field.dtype)
    for s in range(tones):
        piece = lax.dynamic_slice_in_dim(field, (tone + s) % tones * rows, rows, 0)
        if s:
            piece = lax.ppermute(piece, AXES, chain.shift(s))
        slot = turned(tones, place, (tone - s) % tones)
        chunks = lax.dynamic_update_slice_in_dim(chunks, piece, slot * width, 1)
    half = tones // 2 * width
    low, high = chunks[:, :half], chunks[:, half:]
    keep = jnp.where(core == 0, low, high)
    give = jnp.where(core == 0, high, low)
    got = lax.ppermute(give, AXES, chain.swap())
    even, odd = jnp.where(core == 0, keep, got), jnp.where(core == 0, got, keep)
    parts = []
    for h in range(tones // 2):
        parts += [even[:, h * width : (h + 1) * width], odd[:, h * width : (h + 1) * width]]
    return jnp.concatenate(parts, axis=1).reshape(shape)


def edges_of(field):
    take = min(field.shape[1], HALO_B * NB)
    return field[:, field.shape[1] - take :], field[:, :take]


def halos(last, first, up, down):
    width = last.shape[1]
    reach = HALO_B * NB
    left, right = [], []
    hop, have = 1, 0
    while have < reach:
        take = min(width, reach - have)
        left.insert(0, lax.ppermute(last[:, width - take :], AXES, up(hop)))
        right.append(lax.ppermute(first[:, :take], AXES, down(hop)))
        have, hop = have + take, hop + 1
    if len(left) == 1:
        return left[0], right[0]
    return jnp.concatenate(left, axis=1), jnp.concatenate(right, axis=1)


def hartley(count):
    grid = jnp.arange(count, dtype=jnp.int32)
    phase = grid[:, None] * grid[None, :] % count
    angle = phase.astype(F32) * (2.0 * math.pi / count)
    return (jnp.cos(angle) + jnp.sin(angle)) / math.sqrt(count)


def halves(value):
    top = value.astype(BF16)
    return top, (value - top.astype(F32)).astype(BF16)


def rounded_halves(value):
    top = lax.reduce_precision(value, exponent_bits=8, mantissa_bits=7)
    return top.astype(BF16), (value - top).astype(BF16)


def two_tone_tables(k1, k2, tones):
    local, half = k2 // tones, k1 // 2
    rows = jnp.arange(half * k2 // 2, dtype=jnp.int32)
    index1 = rows // local % half
    index2 = rows // (local * half) * local + rows % local

    def spread(index, table):
        pick = (index[:, None] == jnp.arange(table.shape[0], dtype=jnp.int32)[None, :]).astype(F32)
        left = jnp.dot(pick, table, precision=EXACT)
        return lax.dot_general(left, pick, (((1,), (1,)), ((), ())), precision=EXACT)

    first, second = hartley(k1), hartley(k2)
    ones = [spread(index1, first[p::2, :half]) for p in range(2)]
    twos = [spread(index2, second[p::2, : k2 // 2]) for p in range(2)]
    forward = jnp.stack([ones[p // 2] * twos[p % 2] for p in range(4)])
    return (*rounded_halves(forward), *rounded_halves(jnp.swapaxes(forward, 1, 2)))


def dot3(a_top, a_low, b_top, b_low):
    def dot(a, b):
        return jnp.dot(a, b, preferred_element_type=F32)

    return dot(a_top, b_top) + (dot(a_top, b_low) + dot(a_low, b_top))


def lane_of(row, index):
    lanes = lax.broadcasted_iota(jnp.int32, row.shape, 1)
    return jnp.sum(jnp.where(lanes == index, row, 0.0), axis=1, keepdims=True)


def coefficients(parts):
    columns, norms = [], []
    for j, part in enumerate(parts):
        row = jnp.sum(part[...], axis=0)
        norms.append(lane_of(row, j + 2))
        squared = lane_of(row, j + 1)
        columns.append(
            ([lane_of(row, i) / norms[i] for i in range(j + 1)], squared, lax.rsqrt(squared))
        )
    return columns, norms


def orthogonal(raw, vectors, column):
    coeffs, _, scale = column
    for coeff, vector in zip(coeffs, vectors):
        raw = raw - coeff * vector
    return raw * scale


def pieces_of(k1, tones, rows):
    local = rows // (k1 * tones)
    size = k1 // 2 * local
    groups = []
    for a in range(2):
        for b in range(2):
            groups.append(
                [
                    slice(at, at + size)
                    for t in range(tones // 2)
                    for at in [((a * (tones // 2) + t) * k1 + b * (k1 // 2)) * local]
                ]
            )
    return groups


def to_samples(fields, tables, finish):
    top, low = tables[:2]
    sums = [fields[0] + fields[1], fields[2] + fields[3]]
    gaps = [fields[0] - fields[1], fields[2] - fields[3]]
    mixed = [sums[0] + sums[1], sums[0] - sums[1], gaps[0] + gaps[1], gaps[0] - gaps[1]]
    for parity in range(4):
        finish(parity, dot3(top[parity], low[parity], *halves(mixed[parity])))


def to_harmonics(samples, tables):
    top, low = tables[2:]
    parts = [dot3(top[p], low[p], *samples[p]) for p in range(4)]
    even = [parts[0] + parts[1], parts[0] - parts[1]]
    odd = [parts[2] + parts[3], parts[2] - parts[3]]
    return [even[0] + odd[0], even[0] - odd[0], even[1] + odd[1], even[1] - odd[1]]


def taken(value, groups):
    picked = [[value[here, :] for here in group] for group in groups]
    return [p[0] if len(p) == 1 else jnp.concatenate(p, axis=0) for p in picked]


def put(ref, groups, values):
    for group, value in zip(groups, values):
        size = value.shape[0] // len(group)
        for index, here in enumerate(group):
            ref[here, :] = value[index * size : (index + 1) * size, :]


def start_kernel(groups, volts, params, *refs):
    tables, (slope, back) = refs[:4], refs[4:]
    linear, amplitude, sharpness = params[0:1, :], params[1:2, :], params[2:3, :]
    samples = [None] * 4

    def finish(parity, wave):
        size = wave.shape[0]
        bend = jnp.tanh(sharpness * wave)
        here = slice(parity * size, (parity + 1) * size)
        slope[here, :] = linear + amplitude * sharpness * (1.0 - bend * bend)
        samples[parity] = halves(linear * wave + amplitude * bend)

    to_samples(taken(volts, groups), tables, finish)
    put(back, groups, to_harmonics(samples, tables))


def tone_kernel(groups, n_parts, *refs):
    parts, refs = refs[:n_parts], refs[n_parts:]
    raw, basis, refs = refs[0], refs[1 : 1 + n_parts], refs[1 + n_parts :]
    slope, tables, outs = refs[0], refs[1:5], refs[5:]
    fields = taken(raw, groups)
    if n_parts:
        columns, _ = coefficients(parts)
        vectors = [taken(b, groups) for b in basis]
        fields = [
            orthogonal(fields[p], [v[p] for v in vectors], columns[-1]) for p in range(4)
        ]
        put(outs[0], groups, fields)
    samples = [None] * 4

    def finish(parity, wave):
        size = wave.shape[0]
        samples[parity] = halves(slope[parity * size : (parity + 1) * size, :] * wave)

    to_samples(fields, tables, finish)
    put(outs[-1], groups, to_harmonics(samples, tables))


def column_block(width):
    return width // 2 if width % 256 == 0 else width


def columns_call(kernel, parts, fields, small, tables, outs):
    rows, width = fields[0].shape
    block = column_block(width)
    whole = pl.BlockSpec((rows, block), lambda i: (0, i))
    once = functools.partial(pl.BlockSpec, pipeline_mode=pl.Buffered(1))
    specs = [once(p.shape, lambda i: (0, 0, 0)) for p in parts]
    specs += [whole for _ in fields]
    specs += [pl.BlockSpec((s.shape[0], block), lambda i: (0, i)) for s in small]
    specs += [once(t.shape, lambda i: (0, 0, 0)) for t in tables]
    return pl.pallas_call(
        kernel,
        grid=(width // block,),
        in_specs=specs,
        out_specs=[whole] * outs,
        out_shape=[jax.ShapeDtypeStruct((rows, width), F32)] * outs,
        compiler_params=pltpu.CompilerParams(vmem_limit_bytes=LIMIT),
        cost_estimate=pl.CostEstimate(
            flops=3 * rows * rows * width, bytes_accessed=16 * rows * width, transcendentals=0
        ),
    )(*parts, *fields, *small, *tables)


def coupled(left, field, right, op_top, op_low, ext, write):
    block, width = field.shape
    reach = HALO_B * NB
    for value, at in ((left, 0), (field, reach), (right, reach + width)):
        here = slice(at, at + value.shape[1])
        ext[:block, here], ext[block:, here] = halves(value)
    step = 2 * NB if width % (2 * NB) == 0 else NB
    for at in range(0, width, step):
        rows = slice(at, at + step + 2 * reach)
        here = slice(at, at + step)
        both = jnp.dot(ext[:, rows], op_top[rows, here], preferred_element_type=F32)
        rest = jnp.dot(ext[:block, rows], op_low[rows, here], preferred_element_type=F32)
        write(here, both[:block] + (both[block:] + rest))


def residual_kernel(source, volts, left, right, caps, damps, op_top, op_low, out, ext):
    def write(here, value):
        scaled = damps[...] * caps[:, here] * volts[:, here]
        out[:, here] = source[:, here] - (scaled + value)

    coupled(left[...], volts[...], right[...], op_top, op_low, ext, write)


def image_kernel(n_parts, more, *refs):
    parts, refs = refs[:n_parts], refs[n_parts:]
    basis, refs = refs[: n_parts + 1], refs[n_parts + 1 :]
    tones, left, right = refs[0], refs[1][...], refs[2][...]
    lefts, rights = refs[3 : 3 + n_parts], refs[3 + n_parts : 3 + 2 * n_parts]
    refs = refs[3 + 2 * n_parts :]
    caps, damps, op_top, op_low = refs[:4]
    out, stats = refs[4:6]
    refs = refs[6:]
    step = pl.program_id(0)
    if n_parts:
        columns, _ = coefficients(parts)
        left = orthogonal(left, [b[...] for b in lefts], columns[-1])
        right = orthogonal(right, [b[...] for b in rights], columns[-1])
    edges = None
    if more:
        if n_parts:
            refs[0][...] = left
            refs[1][...] = right
            refs = refs[2:]
        edges, refs = refs[:2], refs[2:]
    ext, sums = refs
    field = basis[-1]

    @pl.when(step == 0)
    def _():
        sums[...] = jnp.zeros_like(sums)

    def tile_sum(value):
        value = jnp.sum(value.reshape(value.shape[0] // 8, 8, value.shape[1]), axis=0)
        total = value[:, :NB]
        for at in range(NB, value.shape[1], NB):
            total = total + value[:, at : at + NB]
        return total

    def write(here, value):
        mine = field[:, here]
        value = value + (tones[:, here] + damps[...] * caps[:, here] * mine)
        out[:, here] = value
        for i in range(n_parts + 1):
            sums[i] += tile_sum(basis[i][:, here] * value)
        sums[n_parts + 1] += tile_sum(value * value)
        sums[n_parts + 2] += tile_sum(mine * mine)

    coupled(left, field[...], right, op_top, op_low, ext, write)

    if edges:
        take = edges[0].shape[1]
        edges[0][...] = out[:, out.shape[1] - take :]
        edges[1][...] = out[:, :take]

    @pl.when(step == pl.num_programs(0) - 1)
    def _():
        lanes = lax.broadcasted_iota(jnp.int32, (1, NB), 1)
        row = jnp.zeros((1, NB), F32)
        for i in range(n_parts + 3):
            total = jnp.sum(jnp.sum(sums[i], axis=0, keepdims=True), axis=1, keepdims=True)
            row = jnp.where(lanes == i, total, row)
        stats[...] = jnp.broadcast_to(row[None], stats.shape)


def rows_call(kernel, parts, fields, caps, damps, operator, outs, stats, scratch, limit=LIMIT):
    rows, width = fields[0].shape
    block = min(rows, ROWS)
    once = functools.partial(pl.BlockSpec, pipeline_mode=pl.Buffered(1))

    def along(shape):
        return pl.BlockSpec((block, shape[1]), lambda i: (i, 0))

    specs = [once(p.shape, lambda i: (0, 0, 0)) for p in parts]
    specs += [along(f.shape) for f in fields]
    small = []
    if caps is not None:
        specs += [once(caps.shape, lambda i: (0, 0)), along(damps.shape)]
        small += [caps, damps]
    specs += [once(o.shape, lambda i: (0, 0)) for o in operator]
    shapes = [jax.ShapeDtypeStruct(o, F32) for o in outs]
    out_specs = [along(o) for o in outs]
    if stats:
        shapes.insert(1, jax.ShapeDtypeStruct((stats, 1, NB), F32))
        out_specs.insert(1, pl.BlockSpec((stats, 1, NB), lambda i: (0, 0, 0)))
    flops = 12 * rows * width * (width + HALO_B * NB) if operator else 16 * rows * width
    return pl.pallas_call(
        kernel,
        grid=(rows // block,),
        in_specs=specs,
        out_specs=out_specs,
        out_shape=shapes,
        scratch_shapes=scratch(block),
        compiler_params=pltpu.CompilerParams(vmem_limit_bytes=limit),
        cost_estimate=pl.CostEstimate(
            flops=flops, bytes_accessed=4 * rows * width * len(fields), transcendentals=0
        ),
    )(*parts, *fields, *small, *operator)


def operator_kernel(band_code, active, coupling, top, low):
    blocks = coupling.shape[0]
    for block in range(blocks):
        cols = slice(block * NB, (block + 1) * NB)
        for row in range(blocks + 2 * HALO_B):
            here = slice(row * NB, (row + 1) * NB)
            offset = row - block
            if 0 <= offset < NOFF:
                band = 0
                for j in range(NOFF):
                    band = band + jnp.where(band_code[j] == offset, j, 0)
                value = jnp.transpose(coupling[block, band]) * active[block, band]
                top[here, cols], low[here, cols] = halves(value)
            else:
                top[here, cols] = jnp.zeros((NB, NB), BF16)
                low[here, cols] = jnp.zeros((NB, NB), BF16)


def band_operator(coupling, band_code, active):
    blocks = coupling.shape[0]
    shape = ((blocks + 2 * HALO_B) * NB, blocks * NB)
    smem = pl.BlockSpec(memory_space=pltpu.SMEM)
    vmem = pl.BlockSpec(memory_space=pltpu.VMEM)
    return pl.pallas_call(
        operator_kernel,
        name="operator",
        in_specs=[smem, smem, vmem],
        out_specs=[vmem, vmem],
        out_shape=[jax.ShapeDtypeStruct(shape, BF16)] * 2,
        compiler_params=pltpu.CompilerParams(vmem_limit_bytes=LIMIT),
        cost_estimate=pl.CostEstimate(flops=1 << 22, bytes_accessed=1 << 22, transcendentals=0),
    )(band_code, active, coupling)


def solve(gram, rhs):
    count = len(rhs)
    lower = [[None] * count for _ in range(count)]
    for i in range(count):
        for j in range(i + 1):
            total = gram[i][j]
            for k in range(j):
                total = total - lower[i][k] * lower[j][k]
            lower[i][j] = jnp.sqrt(total) if i == j else total / lower[j][j]
    forward = []
    for i in range(count):
        total = rhs[i]
        for k in range(i):
            total = total - lower[i][k] * forward[k]
        forward.append(total / lower[i][i])
    backward = [None] * count
    for i in reversed(range(count)):
        total = forward[i]
        for k in range(i + 1, count):
            total = total - lower[k][i] * backward[k]
        backward[i] = total / lower[i][i]
    return backward


def answer_of(parts):
    columns, norms = coefficients(parts)
    hessen = [[None] * M for _ in range(M + 1)]
    for j, (coeffs, squared, scale) in enumerate(columns):
        for i in range(j + 1):
            hessen[i][j] = coeffs[i]
        hessen[j + 1][j] = squared * scale
    gram = [[None] * M for _ in range(M)]
    for j in range(M):
        for i in range(j):
            total = norms[0] * hessen[0][i] * hessen[0][j]
            for k in range(1, i + 2):
                total = total + norms[k] * hessen[k][i] * hessen[k][j]
            gram[j][i] = total
        gram[j][j] = columns[j][1]
    answer = solve(gram, [norms[0] * hessen[0][j] for j in range(M)])
    fitted = []
    for i in range(M):
        first = max(i - 1, 0)
        total = hessen[i][first] * answer[first]
        for j in range(first + 1, M - 1):
            total = total + hessen[i][j] * answer[j]
        fitted.append(total)
    return answer, fitted


def final_kernel(*refs):
    parts, basis, (volts, image, updated, remaining) = refs[:M], refs[M : 2 * M], refs[2 * M :]
    answer, fitted = answer_of(parts)
    total = answer[0] * basis[0][...]
    rest = basis[0][...] - fitted[0] * basis[0][...]
    for j in range(1, M):
        vector = basis[j][...]
        total = total + answer[j] * vector
        rest = rest - fitted[j] * vector
    updated[...] = volts[...] + total
    remaining[...] = rest - answer[M - 1] * image[...]


def make(nodes, tones):
    chain = Chain(nodes, tones)
    count = nodes * tones

    def per_device(voltages, source, coupling, band_code, active, cap, damp, kind, type_params):
        node, tone = lax.axis_index("node"), lax.axis_index("tone")
        place = {"tone": tone, "group": node // 2, "core": node % 2}
        place["turn"] = turned(tones, place, tone)
        shape = voltages.shape
        k1, k2 = shape[0], shape[1] * tones

        volts = gather_tones(chain, voltages, place)
        rows, width = volts.shape
        local = rows // tones

        onehot = (kind[None, :] == jnp.arange(NTYPES, dtype=jnp.int32)[:, None]).astype(F32)
        per_node = jnp.dot(type_params, onehot, precision=EXACT)
        per_node = jnp.concatenate(
            [per_node, cap[None, :], jnp.zeros((4, cap.shape[0]), F32)], axis=0
        )
        per_node = chunk_of(chain, per_node, place, 1)
        damps = jnp.zeros((tones, local, 1), F32)
        for s in range(tones):
            piece = lax.ppermute(damp, AXES, chain.shift(s)) if s else damp
            piece = piece.reshape(1, local, 1)
            damps = lax.dynamic_update_slice_in_dim(damps, piece, (tone - s) % tones, 0)
        damps = damps.reshape(rows, 1)

        def ext_scratch(nodes):
            ext = nodes + 2 * HALO_B * NB
            return lambda block: [pltpu.VMEM((2 * block, ext), BF16)]

        volts_here = voltages.reshape(local, shape[2])
        left, right = halos(*edges_of(volts_here), chain.node_up, chain.node_down)
        (driven,) = rows_call(
            residual_kernel,
            [],
            [source.reshape(local, shape[2]), volts_here, left, right],
            cap[None, :],
            damp.reshape(local, 1),
            band_operator(coupling, band_code, active.astype(F32)),
            [(local, shape[2])],
            0,
            ext_scratch(shape[2]),
            LIMIT_START,
        )
        mine = chunk_of(chain, coupling, place, 0)
        mine_active = chunk_of(chain, active.astype(F32), place, 0)
        driven, damps, mine_active, per_node = lax.optimization_barrier(
            (driven, damps, mine_active, per_node)
        )
        caps = per_node[3:4]
        driven = gather_tones(chain, driven.reshape(shape), place)

        operator = band_operator(mine, band_code, mine_active)
        tables = two_tone_tables(k1, k2, tones)
        groups = pieces_of(k1, tones, rows)

        slope, back = columns_call(
            functools.partial(start_kernel, groups), [], [volts], [per_node], tables, 2
        )
        start = driven - back

        left, right = halos(*edges_of(start), chain.up, chain.down)
        basis, lefts, rights, parts = [], [], [], []
        image = start
        edge, reach = (rows, min(width, HALO_B * NB)), (rows, HALO_B * NB)
        for column in range(M):
            made = columns_call(
                functools.partial(tone_kernel, groups, column),
                parts,
                [image, *basis, slope],
                [],
                tables,
                2 if column else 1,
            )
            new, toned = made if column else (start, made[0])
            more = column + 1 < M
            made = rows_call(
                functools.partial(image_kernel, column, more),
                parts,
                [*basis, new, toned, left, right, *lefts, *rights],
                caps,
                damps,
                operator,
                [(rows, width)] + ([reach, reach] if more and column else []) + [edge, edge] * more,
                count,
                lambda block, n=column: ext_scratch(width)(block)
                + [pltpu.VMEM((n + 3, 8, NB), F32)],
            )
            image, stats = made[:2]
            basis.append(new)
            if more:
                lefts.append(made[2] if column else left)
                rights.append(made[3] if column else right)
                left, right = halos(*made[-2:], chain.up, chain.down)
            part = lax.all_to_all(stats, AXES, 0, 0, tiled=True)
            parts = parts + [part]

        new_volts, remaining = rows_call(
            final_kernel,
            parts,
            [*basis, volts, image],
            None,
            None,
            [],
            [(rows, width)] * 2,
            0,
            lambda block: [],
            LIMIT_END,
        )
        new_volts = scatter_tones(chain, new_volts, place, shape)
        remaining = scatter_tones(chain, remaining, place, shape)
        return new_volts, remaining

    return per_device


def solution(mesh):
    placed = (
        P(None, "tone", "node"),
        P(None, "tone", "node"),
        P("node", None, None, None),
        P(),
        P("node", None),
        P("node"),
        P(None, "tone"),
        P("node"),
        P(),
    )
    body = make(mesh.shape["node"], mesh.shape["tone"])

    return jax.shard_map(
        body,
        mesh=mesh,
        in_specs=placed,
        out_specs=(P(None, "tone", "node"), P(None, "tone", "node")),
        check_vma=False,
    )
```

```python
import functools
import math

import jax
import jax.numpy as jnp
from jax import lax
from jax.experimental import pallas as pl
from jax.experimental.pallas import tpu as pltpu
from jax.sharding import PartitionSpec as P

NB = 128
HALO_B = 3
NOFF = 7
M = 4
NTYPES = 4
AXES = ("node", "tone")
EXACT = lax.Precision.HIGHEST
F32 = jnp.float32
BF16 = jnp.bfloat16
LIMIT = 16 * 1024 * 1024
LIMIT_START = 60 * 1024 * 1024
LIMIT_END = 60 * 1024 * 1024
ROWS = 256


class Chain:
    def __init__(self, nodes, tones):
        self.nodes, self.tones = nodes, tones
        self.at = [0] * (nodes * tones)
        for i in range(nodes):
            for t in range(tones):
                place = (i // 2) * 2 * tones + 2 * self.turn(i, t) + i % 2
                self.at[place] = i * tones + t

    def turn(self, i, t):
        return t if (i // 2) % 2 == 0 else self.tones - 1 - t

    def device(self, group, core, turn):
        return self.at[group * 2 * self.tones + 2 * turn + core]

    def up(self, hop):
        return [(self.at[p], self.at[p + hop]) for p in range(len(self.at) - hop)]

    def down(self, hop):
        return [(b, a) for a, b in self.up(hop)]

    def node_up(self, hop):
        tones = self.tones
        return [
            (i * tones + t, (i + hop) * tones + t)
            for i in range(self.nodes - hop)
            for t in range(tones)
        ]

    def node_down(self, hop):
        return [(b, a) for a, b in self.node_up(hop)]

    def swap(self):
        tones = self.tones
        return [(i * tones + t, (i ^ 1) * tones + t) for i in range(self.nodes) for t in range(tones)]

    def shift(self, s):
        tones = self.tones
        return [
            (i * tones + t, i * tones + (t + s) % tones)
            for i in range(self.nodes)
            for t in range(tones)
        ]

    def first(self):
        pairs = []
        for g in range(self.nodes // 2):
            for a, b in (((0, 0), (1, 0)), ((0, 1), (0, 0)), ((1, 0), (1, 1)), ((1, 1), (0, 1))):
                pairs.append((self.device(g, *a), self.device(g, *b)))
        return pairs

    def second(self):
        pairs = []
        for g in range(self.nodes // 2):
            for a, b in (((0, 1), (1, 0)), ((1, 0), (0, 1))):
                pairs.append((self.device(g, *a), self.device(g, *b)))
        return pairs


def flipped(pairs):
    return [(b, a) for a, b in pairs]


def turned(tones, place, index):
    return jnp.where((place["group"] % 2) == 0, index, tones - 1 - index)


def parity_chunks(value, tones, parity, axis):
    width = value.shape[axis] // tones
    parts = [
        lax.dynamic_slice_in_dim(value, (2 * h + parity) * width, width, axis)
        for h in range(tones // 2)
    ]
    return parts[0] if len(parts) == 1 else jnp.concatenate(parts, axis=axis)


def core_swap(chain, value, core, axis):
    keep = parity_chunks(value, chain.tones, core, axis)
    give = parity_chunks(value, chain.tones, 1 - core, axis)
    got = lax.ppermute(give, AXES, chain.swap())
    return jnp.where(core == 0, keep, got), jnp.where(core == 0, got, keep)


def chunk_of(chain, value, place, axis):
    low, high = core_swap(chain, value, place["core"], axis)
    half = chain.tones // 2
    both = jnp.where(place["turn"] < half, low, high)
    width = value.shape[axis] // chain.tones
    return lax.dynamic_slice_in_dim(both, place["turn"] % half * width, width, axis)


def gather_tones(chain, field, place):
    tones, tone, core, turn = chain.tones, place["tone"], place["core"], place["turn"]
    width = field.shape[2] // tones
    rows = field.shape[0] * field.shape[1]
    field = field.reshape(rows, field.shape[2])
    if tones == 2:
        one = lax.dynamic_slice_in_dim(field, (1 - turn) * width, width, 1)
        two = lax.dynamic_slice_in_dim(field, turn * width, width, 1)
        got_one = lax.ppermute(one, AXES, chain.first())
        got_two = lax.ppermute(two, AXES, chain.second())
        same = jnp.where(core == turn, two, got_one)
        other = jnp.where(core == turn, got_one, got_two)
        return jnp.concatenate(
            [jnp.where(tone == 0, same, other), jnp.where(tone == 0, other, same)], axis=0
        )
    low, high = core_swap(chain, field, core, 1)
    chunks = jnp.concatenate([low, high], axis=1)
    out = jnp.zeros((tones * rows, width), field.dtype)
    for s in range(tones):
        target = turned(tones, place, (tone + s) % tones)
        piece = lax.dynamic_slice_in_dim(chunks, target * width, width, 1)
        if s:
            piece = lax.ppermute(piece, AXES, chain.shift(s))
        out = lax.dynamic_update_slice_in_dim(out, piece, (tone - s) % tones * rows, 0)
    return out


def scatter_tones(chain, field, place, shape):
    tones, tone, core, turn = chain.tones, place["tone"], place["core"], place["turn"]
    width = field.shape[1]
    rows = field.shape[0] // tones
    if tones == 2:
        same = lax.dynamic_slice_in_dim(field, tone * rows, rows, 0)
        other = lax.dynamic_slice_in_dim(field, (1 - tone) * rows, rows, 0)
        one = jnp.where(core == turn, other, same)
        got_one = lax.ppermute(one, AXES, flipped(chain.first()))
        got_two = lax.ppermute(other, AXES, flipped(chain.second()))
        at_turn = jnp.where(core == turn, same, got_two)
        return jnp.where(
            turn == 0,
            jnp.concatenate([at_turn, got_one], axis=1),
            jnp.concatenate([got_one, at_turn], axis=1),
        ).reshape(shape)
    chunks = jnp.zeros((rows, tones * width), field.dtype)
    for s in range(tones):
        piece = lax.dynamic_slice_in_dim(field, (tone + s) % tones * rows, rows, 0)
        if s:
            piece = lax.ppermute(piece, AXES, chain.shift(s))
        slot = turned(tones, place, (tone - s) % tones)
        chunks = lax.dynamic_update_slice_in_dim(chunks, piece, slot * width, 1)
    half = tones // 2 * width
    low, high = chunks[:, :half], chunks[:, half:]
    keep = jnp.where(core == 0, low, high)
    give = jnp.where(core == 0, high, low)
    got = lax.ppermute(give, AXES, chain.swap())
    even, odd = jnp.where(core == 0, keep, got), jnp.where(core == 0, got, keep)
    parts = []
    for h in range(tones // 2):
        parts += [even[:, h * width : (h + 1) * width], odd[:, h * width : (h + 1) * width]]
    return jnp.concatenate(parts, axis=1).reshape(shape)


def edges_of(field):
    take = min(field.shape[1], HALO_B * NB)
    return field[:, field.shape[1] - take :], field[:, :take]


def halos(last, first, up, down):
    width = last.shape[1]
    reach = HALO_B * NB
    left, right = [], []
    hop, have = 1, 0
    while have < reach:
        take = min(width, reach - have)
        left.insert(0, lax.ppermute(last[:, width - take :], AXES, up(hop)))
        right.append(lax.ppermute(first[:, :take], AXES, down(hop)))
        have, hop = have + take, hop + 1
    if len(left) == 1:
        return left[0], right[0]
    return jnp.concatenate(left, axis=1), jnp.concatenate(right, axis=1)


def hartley(count):
    grid = jnp.arange(count, dtype=jnp.int32)
    phase = grid[:, None] * grid[None, :] % count
    angle = phase.astype(F32) * (2.0 * math.pi / count)
    return (jnp.cos(angle) + jnp.sin(angle)) / math.sqrt(count)


def halves(value):
    top = value.astype(BF16)
    return top, (value - top.astype(F32)).astype(BF16)


def rounded_halves(value):
    top = lax.reduce_precision(value, exponent_bits=8, mantissa_bits=7)
    return top.astype(BF16), (value - top).astype(BF16)


def two_tone_tables(k1, k2, tones):
    local, half = k2 // tones, k1 // 2
    rows = jnp.arange(half * k2 // 2, dtype=jnp.int32)
    index1 = rows // local % half
    index2 = rows // (local * half) * local + rows % local

    def spread(index, table):
        pick = (index[:, None] == jnp.arange(table.shape[0], dtype=jnp.int32)[None, :]).astype(F32)
        left = jnp.dot(pick, table, precision=EXACT)
        return lax.dot_general(left, pick, (((1,), (1,)), ((), ())), precision=EXACT)

    first, second = hartley(k1), hartley(k2)
    ones = [spread(index1, first[p::2, :half]) for p in range(2)]
    twos = [spread(index2, second[p::2, : k2 // 2]) for p in range(2)]
    forward = jnp.stack([ones[p // 2] * twos[p % 2] for p in range(4)])
    return (*rounded_halves(forward), *rounded_halves(jnp.swapaxes(forward, 1, 2)))


def dot3(a_top, a_low, b_top, b_low):
    def dot(a, b):
        return jnp.dot(a, b, preferred_element_type=F32)

    return dot(a_top, b_top) + (dot(a_top, b_low) + dot(a_low, b_top))


def lane_of(row, index):
    lanes = lax.broadcasted_iota(jnp.int32, row.shape, 1)
    return jnp.sum(jnp.where(lanes == index, row, 0.0), axis=1, keepdims=True)


def coefficients(parts):
    columns, norms = [], []
    for j, part in enumerate(parts):
        row = jnp.sum(part[...], axis=0)
        norms.append(lane_of(row, j + 2))
        squared = lane_of(row, j + 1)
        columns.append(
            ([lane_of(row, i) / norms[i] for i in range(j + 1)], squared, lax.rsqrt(squared))
        )
    return columns, norms


def orthogonal(raw, vectors, column):
    coeffs, _, scale = column
    for coeff, vector in zip(coeffs, vectors):
        raw = raw - coeff * vector
    return raw * scale


def pieces_of(k1, tones, rows):
    local = rows // (k1 * tones)
    size = k1 // 2 * local
    groups = []
    for a in range(2):
        for b in range(2):
            groups.append(
                [
                    slice(at, at + size)
                    for t in range(tones // 2)
                    for at in [((a * (tones // 2) + t) * k1 + b * (k1 // 2)) * local]
                ]
            )
    return groups


def to_samples(fields, tables, finish):
    top, low = tables[:2]
    sums = [fields[0] + fields[1], fields[2] + fields[3]]
    gaps = [fields[0] - fields[1], fields[2] - fields[3]]
    mixed = [sums[0] + sums[1], sums[0] - sums[1], gaps[0] + gaps[1], gaps[0] - gaps[1]]
    for parity in range(4):
        finish(parity, dot3(top[parity], low[parity], *halves(mixed[parity])))


def to_harmonics(samples, tables):
    top, low = tables[2:]
    parts = [dot3(top[p], low[p], *samples[p]) for p in range(4)]
    even = [parts[0] + parts[1], parts[0] - parts[1]]
    odd = [parts[2] + parts[3], parts[2] - parts[3]]
    return [even[0] + odd[0], even[0] - odd[0], even[1] + odd[1], even[1] - odd[1]]


def taken(value, groups):
    picked = [[value[here, :] for here in group] for group in groups]
    return [p[0] if len(p) == 1 else jnp.concatenate(p, axis=0) for p in picked]


def put(ref, groups, values):
    for group, value in zip(groups, values):
        size = value.shape[0] // len(group)
        for index, here in enumerate(group):
            ref[here, :] = value[index * size : (index + 1) * size, :]


def start_kernel(groups, volts, params, *refs):
    tables, (slope, back) = refs[:4], refs[4:]
    linear, amplitude, sharpness = params[0:1, :], params[1:2, :], params[2:3, :]
    samples = [None] * 4

    def finish(parity, wave):
        size = wave.shape[0]
        bend = jnp.tanh(sharpness * wave)
        here = slice(parity * size, (parity + 1) * size)
        slope[here, :] = linear + amplitude * sharpness * (1.0 - bend * bend)
        samples[parity] = halves(linear * wave + amplitude * bend)

    to_samples(taken(volts, groups), tables, finish)
    put(back, groups, to_harmonics(samples, tables))


def tone_kernel(groups, n_parts, *refs):
    parts, refs = refs[:n_parts], refs[n_parts:]
    raw, basis, refs = refs[0], refs[1 : 1 + n_parts], refs[1 + n_parts :]
    slope, tables, outs = refs[0], refs[1:5], refs[5:]
    fields = taken(raw, groups)
    if n_parts:
        columns, _ = coefficients(parts)
        vectors = [taken(b, groups) for b in basis]
        fields = [
            orthogonal(fields[p], [v[p] for v in vectors], columns[-1]) for p in range(4)
        ]
        put(outs[0], groups, fields)
    samples = [None] * 4

    def finish(parity, wave):
        size = wave.shape[0]
        samples[parity] = halves(slope[parity * size : (parity + 1) * size, :] * wave)

    to_samples(fields, tables, finish)
    put(outs[-1], groups, to_harmonics(samples, tables))


def column_block(width):
    return width // 2 if width % 256 == 0 else width


def columns_call(kernel, parts, fields, small, tables, outs):
    rows, width = fields[0].shape
    block = column_block(width)
    whole = pl.BlockSpec((rows, block), lambda i: (0, i))
    once = functools.partial(pl.BlockSpec, pipeline_mode=pl.Buffered(1))
    specs = [once(p.shape, lambda i: (0, 0, 0)) for p in parts]
    specs += [whole for _ in fields]
    specs += [pl.BlockSpec((s.shape[0], block), lambda i: (0, i)) for s in small]
    specs += [once(t.shape, lambda i: (0, 0, 0)) for t in tables]
    return pl.pallas_call(
        kernel,
        grid=(width // block,),
        in_specs=specs,
        out_specs=[whole] * outs,
        out_shape=[jax.ShapeDtypeStruct((rows, width), F32)] * outs,
        compiler_params=pltpu.CompilerParams(vmem_limit_bytes=LIMIT),
        cost_estimate=pl.CostEstimate(
            flops=3 * rows * rows * width, bytes_accessed=16 * rows * width, transcendentals=0
        ),
    )(*parts, *fields, *small, *tables)


def coupled(left, field, right, op_top, op_low, ext, write):
    block, width = field.shape
    reach = HALO_B * NB
    for value, at in ((left, 0), (field, reach), (right, reach + width)):
        here = slice(at, at + value.shape[1])
        ext[:block, here], ext[block:, here] = halves(value)
    step = 2 * NB if width % (2 * NB) == 0 else NB
    for at in range(0, width, step):
        rows = slice(at, at + step + 2 * reach)
        here = slice(at, at + step)
        both = jnp.dot(ext[:, rows], op_top[rows, here], preferred_element_type=F32)
        rest = jnp.dot(ext[:block, rows], op_low[rows, here], preferred_element_type=F32)
        write(here, both[:block] + (both[block:] + rest))


def residual_kernel(source, volts, left, right, caps, damps, op_top, op_low, out, ext):
    def write(here, value):
        scaled = damps[...] * caps[:, here] * volts[:, here]
        out[:, here] = source[:, here] - (scaled + value)

    coupled(left[...], volts[...], right[...], op_top, op_low, ext, write)


def image_kernel(n_parts, more, *refs):
    parts, refs = refs[:n_parts], refs[n_parts:]
    basis, refs = refs[: n_parts + 1], refs[n_parts + 1 :]
    tones, left, right = refs[0], refs[1][...], refs[2][...]
    lefts, rights = refs[3 : 3 + n_parts], refs[3 + n_parts : 3 + 2 * n_parts]
    refs = refs[3 + 2 * n_parts :]
    caps, damps, op_top, op_low = refs[:4]
    out, stats = refs[4:6]
    refs = refs[6:]
    step = pl.program_id(0)
    if n_parts:
        columns, _ = coefficients(parts)
        left = orthogonal(left, [b[...] for b in lefts], columns[-1])
        right = orthogonal(right, [b[...] for b in rights], columns[-1])
    edges = None
    if more:
        if n_parts:
            refs[0][...] = left
            refs[1][...] = right
            refs = refs[2:]
        edges, refs = refs[:2], refs[2:]
    ext, sums = refs
    field = basis[-1]

    @pl.when(step == 0)
    def _():
        sums[...] = jnp.zeros_like(sums)

    def tile_sum(value):
        value = jnp.sum(value.reshape(value.shape[0] // 8, 8, value.shape[1]), axis=0)
        total = value[:, :NB]
        for at in range(NB, value.shape[1], NB):
            total = total + value[:, at : at + NB]
        return total

    def write(here, value):
        mine = field[:, here]
        value = value + (tones[:, here] + damps[...] * caps[:, here] * mine)
        out[:, here] = value
        for i in range(n_parts + 1):
            sums[i] += tile_sum(basis[i][:, here] * value)
        sums[n_parts + 1] += tile_sum(value * value)
        sums[n_parts + 2] += tile_sum(mine * mine)

    coupled(left, field[...], right, op_top, op_low, ext, write)

    if edges:
        take = edges[0].shape[1]
        edges[0][...] = out[:, out.shape[1] - take :]
        edges[1][...] = out[:, :take]

    @pl.when(step == pl.num_programs(0) - 1)
    def _():
        lanes = lax.broadcasted_iota(jnp.int32, (1, NB), 1)
        row = jnp.zeros((1, NB), F32)
        for i in range(n_parts + 3):
            total = jnp.sum(jnp.sum(sums[i], axis=0, keepdims=True), axis=1, keepdims=True)
            row = jnp.where(lanes == i, total, row)
        stats[...] = jnp.broadcast_to(row[None], stats.shape)


def rows_call(kernel, parts, fields, caps, damps, operator, outs, stats, scratch, limit=LIMIT):
    rows, width = fields[0].shape
    block = min(rows, ROWS if operator else ROWS // 2)
    once = functools.partial(pl.BlockSpec, pipeline_mode=pl.Buffered(1))

    def along(shape):
        return pl.BlockSpec((block, shape[1]), lambda i: (i, 0))

    specs = [once(p.shape, lambda i: (0, 0, 0)) for p in parts]
    specs += [along(f.shape) for f in fields]
    small = []
    if caps is not None:
        specs += [once(caps.shape, lambda i: (0, 0)), along(damps.shape)]
        small += [caps, damps]
    specs += [once(o.shape, lambda i: (0, 0)) for o in operator]
    shapes = [jax.ShapeDtypeStruct(o, F32) for o in outs]
    out_specs = [along(o) for o in outs]
    if stats:
        shapes.insert(1, jax.ShapeDtypeStruct((stats, 1, NB), F32))
        out_specs.insert(1, pl.BlockSpec((stats, 1, NB), lambda i: (0, 0, 0)))
    flops = 12 * rows * width * (width + HALO_B * NB) if operator else 16 * rows * width
    return pl.pallas_call(
        kernel,
        grid=(rows // block,),
        in_specs=specs,
        out_specs=out_specs,
        out_shape=shapes,
        scratch_shapes=scratch(block),
        compiler_params=pltpu.CompilerParams(vmem_limit_bytes=limit),
        cost_estimate=pl.CostEstimate(
            flops=flops, bytes_accessed=4 * rows * width * len(fields), transcendentals=0
        ),
    )(*parts, *fields, *small, *operator)


def operator_kernel(band_code, active, coupling, top, low):
    blocks = coupling.shape[0]
    for block in range(blocks):
        cols = slice(block * NB, (block + 1) * NB)
        for row in range(blocks + 2 * HALO_B):
            here = slice(row * NB, (row + 1) * NB)
            offset = row - block
            if 0 <= offset < NOFF:
                band = 0
                for j in range(NOFF):
                    band = band + jnp.where(band_code[j] == offset, j, 0)
                value = jnp.transpose(coupling[block, band]) * active[block, band]
                top[here, cols], low[here, cols] = halves(value)
            else:
                top[here, cols] = jnp.zeros((NB, NB), BF16)
                low[here, cols] = jnp.zeros((NB, NB), BF16)


def band_operator(coupling, band_code, active):
    blocks = coupling.shape[0]
    shape = ((blocks + 2 * HALO_B) * NB, blocks * NB)
    smem = pl.BlockSpec(memory_space=pltpu.SMEM)
    vmem = pl.BlockSpec(memory_space=pltpu.VMEM)
    return pl.pallas_call(
        operator_kernel,
        name="operator",
        in_specs=[smem, smem, vmem],
        out_specs=[vmem, vmem],
        out_shape=[jax.ShapeDtypeStruct(shape, BF16)] * 2,
        compiler_params=pltpu.CompilerParams(vmem_limit_bytes=LIMIT),
        cost_estimate=pl.CostEstimate(flops=1 << 22, bytes_accessed=1 << 22, transcendentals=0),
    )(band_code, active, coupling)


def solve(gram, rhs):
    count = len(rhs)
    lower = [[None] * count for _ in range(count)]
    for i in range(count):
        for j in range(i + 1):
            total = gram[i][j]
            for k in range(j):
                total = total - lower[i][k] * lower[j][k]
            lower[i][j] = jnp.sqrt(total) if i == j else total / lower[j][j]
    forward = []
    for i in range(count):
        total = rhs[i]
        for k in range(i):
            total = total - lower[i][k] * forward[k]
        forward.append(total / lower[i][i])
    backward = [None] * count
    for i in reversed(range(count)):
        total = forward[i]
        for k in range(i + 1, count):
            total = total - lower[k][i] * backward[k]
        backward[i] = total / lower[i][i]
    return backward


def answer_of(parts):
    columns, norms = coefficients(parts)
    hessen = [[None] * M for _ in range(M + 1)]
    for j, (coeffs, squared, scale) in enumerate(columns):
        for i in range(j + 1):
            hessen[i][j] = coeffs[i]
        hessen[j + 1][j] = squared * scale
    gram = [[None] * M for _ in range(M)]
    for j in range(M):
        for i in range(j):
            total = norms[0] * hessen[0][i] * hessen[0][j]
            for k in range(1, i + 2):
                total = total + norms[k] * hessen[k][i] * hessen[k][j]
            gram[j][i] = total
        gram[j][j] = columns[j][1]
    answer = solve(gram, [norms[0] * hessen[0][j] for j in range(M)])
    fitted = []
    for i in range(M):
        first = max(i - 1, 0)
        total = hessen[i][first] * answer[first]
        for j in range(first + 1, M - 1):
            total = total + hessen[i][j] * answer[j]
        fitted.append(total)
    return answer, fitted


def final_kernel(*refs):
    parts, basis, (volts, image, updated, remaining) = refs[:M], refs[M : 2 * M], refs[2 * M :]
    answer, fitted = answer_of(parts)
    total = answer[0] * basis[0][...]
    rest = basis[0][...] - fitted[0] * basis[0][...]
    for j in range(1, M):
        vector = basis[j][...]
        total = total + answer[j] * vector
        rest = rest - fitted[j] * vector
    updated[...] = volts[...] + total
    remaining[...] = rest - answer[M - 1] * image[...]


def make(nodes, tones):
    chain = Chain(nodes, tones)
    count = nodes * tones

    def per_device(voltages, source, coupling, band_code, active, cap, damp, kind, type_params):
        node, tone = lax.axis_index("node"), lax.axis_index("tone")
        place = {"tone": tone, "group": node // 2, "core": node % 2}
        place["turn"] = turned(tones, place, tone)
        shape = voltages.shape
        k1, k2 = shape[0], shape[1] * tones

        volts = gather_tones(chain, voltages, place)
        rows, width = volts.shape
        local = rows // tones

        onehot = (kind[None, :] == jnp.arange(NTYPES, dtype=jnp.int32)[:, None]).astype(F32)
        per_node = jnp.dot(type_params, onehot, precision=EXACT)
        per_node = jnp.concatenate(
            [per_node, cap[None, :], jnp.zeros((4, cap.shape[0]), F32)], axis=0
        )
        per_node = chunk_of(chain, per_node, place, 1)
        damps = jnp.zeros((tones, local, 1), F32)
        for s in range(tones):
            piece = lax.ppermute(damp, AXES, chain.shift(s)) if s else damp
            piece = piece.reshape(1, local, 1)
            damps = lax.dynamic_update_slice_in_dim(damps, piece, (tone - s) % tones, 0)
        damps = damps.reshape(rows, 1)

        def ext_scratch(nodes):
            ext = nodes + 2 * HALO_B * NB
            return lambda block: [pltpu.VMEM((2 * block, ext), BF16)]

        volts_here = voltages.reshape(local, shape[2])
        left, right = halos(*edges_of(volts_here), chain.node_up, chain.node_down)
        (driven,) = rows_call(
            residual_kernel,
            [],
            [source.reshape(local, shape[2]), volts_here, left, right],
            cap[None, :],
            damp.reshape(local, 1),
            band_operator(coupling, band_code, active.astype(F32)),
            [(local, shape[2])],
            0,
            ext_scratch(shape[2]),
            LIMIT_START,
        )
        mine = chunk_of(chain, coupling, place, 0)
        mine_active = chunk_of(chain, active.astype(F32), place, 0)
        driven, damps, mine_active, per_node = lax.optimization_barrier(
            (driven, damps, mine_active, per_node)
        )
        caps = per_node[3:4]
        driven = gather_tones(chain, driven.reshape(shape), place)

        operator = band_operator(mine, band_code, mine_active)
        tables = two_tone_tables(k1, k2, tones)
        groups = pieces_of(k1, tones, rows)

        slope, back = columns_call(
            functools.partial(start_kernel, groups), [], [volts], [per_node], tables, 2
        )
        start = driven - back

        left, right = halos(*edges_of(start), chain.up, chain.down)
        basis, lefts, rights, parts = [], [], [], []
        image = start
        edge, reach = (rows, min(width, HALO_B * NB)), (rows, HALO_B * NB)
        for column in range(M):
            made = columns_call(
                functools.partial(tone_kernel, groups, column),
                parts,
                [image, *basis, slope],
                [],
                tables,
                2 if column else 1,
            )
            new, toned = made if column else (start, made[0])
            more = column + 1 < M
            made = rows_call(
                functools.partial(image_kernel, column, more),
                parts,
                [*basis, new, toned, left, right, *lefts, *rights],
                caps,
                damps,
                operator,
                [(rows, width)] + ([reach, reach] if more and column else []) + [edge, edge] * more,
                count,
                lambda block, n=column: ext_scratch(width)(block)
                + [pltpu.VMEM((n + 3, 8, NB), F32)],
            )
            image, stats = made[:2]
            basis.append(new)
            if more:
                lefts.append(made[2] if column else left)
                rights.append(made[3] if column else right)
                left, right = halos(*made[-2:], chain.up, chain.down)
            part = lax.all_to_all(stats, AXES, 0, 0, tiled=True)
            parts = parts + [part]

        new_volts, remaining = rows_call(
            final_kernel,
            parts,
            [*basis, volts, image],
            None,
            None,
            [],
            [(rows, width)] * 2,
            0,
            lambda block: [],
            LIMIT_END,
        )
        new_volts = scatter_tones(chain, new_volts, place, shape)
        remaining = scatter_tones(chain, remaining, place, shape)
        return new_volts, remaining

    return per_device


def solution(mesh):
    placed = (
        P(None, "tone", "node"),
        P(None, "tone", "node"),
        P("node", None, None, None),
        P(),
        P("node", None),
        P("node"),
        P(None, "tone"),
        P("node"),
        P(),
    )
    body = make(mesh.shape["node"], mesh.shape["tone"])

    return jax.shard_map(
        body,
        mesh=mesh,
        in_specs=placed,
        out_specs=(P(None, "tone", "node"), P(None, "tone", "node")),
        check_vma=False,
    )
```
